128 devices in a mesh: section: 8 (over y, core), vocab: 16 (over x, z).
Axes of the slice: x: 4, y: 4, z: 4, core: 2. Of those that a mesh axis runs over, the one named last changes fastest.
Arguments:
- stream_in: bfloat16 [128, 5120], P(None, 'vocab'), may hold values from -20 to 20
- deltas: bfloat16 [16, 128, 5120], P('section', None, 'vocab'), may hold values from -6 to 6
- norm_gain: float32 [5120], P('vocab'), may hold values from 0.25 to 1.75
- unembed: bfloat16 [152064, 5120], P(('section', 'vocab')), may hold values from -0.559017 to 0.559017
- targets: int32 [128], replicated, may hold values from 0 to 152063
Outputs:
- lens_lse: float32 [16, 128], P('section')
- lens_entropy: float32 [16, 128], P('section')
- lens_logprob: float32 [16, 128], P('section')
The draws below stay inside these ranges and needn't reach their ends.
All inputs are finite; a program needn't handle non-finite values.
Results may differ from the reference program's by a relative error of at most 0.0077.
Values may be sent and summed in bfloat16 or wider, within the bound.
A program may use at most 128 MiB of HBM per device.

```python
import math
import jax
import jax.numpy as jnp
import numpy as np
from jax import lax

D = 5120
VOCAB = 152064
TOKENS = 128
LAYERS = 16


def draw_unembed(key, part):
    folded = jax.random.fold_in(key, 101)
    key_scale, key_normal = jax.random.split(folded, 2)
    row_scale = jnp.exp(jax.random.uniform(key_scale, (VOCAB, 1), jnp.float32, 0.0, math.log(10.0))) * (0.8 / math.sqrt(D))
    values = jnp.clip(jax.random.normal(key_normal, (VOCAB, D), jnp.float32), -5.0, 5.0) * row_scale
    return values.astype(jnp.bfloat16)


def draw_stream_in(key, part):
    folded = jax.random.fold_in(key, 202)
    key_feature, key_normal = jax.random.split(folded, 2)
    position = jnp.arange(D, dtype=jnp.float32) / D
    feature_scale = 0.5 * jnp.exp(position * math.log(3.0)) * jnp.exp(jax.random.uniform(key_feature, (D,), jnp.float32, 0.0, math.log(3.5)))
    normal_part = jnp.clip(jax.random.normal(key_normal, (TOKENS, D), jnp.float32), -3.5, 3.5)
    values = feature_scale * normal_part
    return jnp.clip(values, -20.0, 20.0).astype(jnp.bfloat16)


def with_ends(result, own_key, least, largest):
    longest = result.shape.index(max(result.shape))
    spots = []
    for shift in (0, 1):
        where = [jax.random.randint(jax.random.fold_in(own_key, axis), (), 0, length) for axis, length in enumerate(result.shape)]
        where[longest] = (where[longest] + shift) % result.shape[longest]
        spots.append(tuple(where))
    return result.at[spots[0]].set(least).at[spots[1]].set(largest)


def level_of(key, extent, cuts, smallest, largest):
    gain = 1.0
    for axis_at, blocks in cuts:
        draws = jax.random.uniform(jax.random.fold_in(jax.random.fold_in(key, 6), axis_at), (blocks,), jnp.float32, smallest / len(cuts), largest / len(cuts))
        gain = gain * jnp.repeat(jnp.exp(draws), extent[axis_at] // blocks).reshape((-1,) + (1,) * (len(extent) - 1 - axis_at))
    return gain


def wide_ids(key, dims, count, skew):
    loads = [min(1 << octave, count + 1 - (1 << octave)) * (1 << 20) // math.isqrt((1 << octave) ** skew) + 1 for octave in range((count + 1).bit_length()) if 1 << octave <= count]
    width = 1 + sum(loads) // (1 << 30)
    grid = np.cumsum(np.array([max(1, weight // width) for weight in loads]))
    lot = jax.random.randint(jax.random.fold_in(key, 1), dims, 0, int(grid[len(loads) - 1]))
    start = jnp.left_shift(1, jnp.searchsorted(jnp.asarray(grid, jnp.int32), lot, side="right").astype(jnp.int32))
    standing = start - 1 + jax.random.randint(jax.random.fold_in(key, 4), dims, 0, 1 << 30) % jnp.minimum(start, count + 1 - start)
    return jax.random.permutation(jax.random.fold_in(key, 2), count)[standing].astype(jnp.int32)


def gaussian(rng, dims, scale, reach, cuts=(), held_as=jnp.bfloat16):
    values = jax.random.normal(rng, dims, jnp.float32) * scale
    if len(cuts) > 0:
        values = level_of(rng, dims, cuts, -0.22, 0.18) * values
    return jnp.clip(values, min=-reach, max=reach).astype(held_as)


def setup_inputs(seed: int = 0) -> dict:
    arg_keys = jax.random.split(jax.random.key(seed), 6)
    stream_in = draw_stream_in(jax.random.fold_in(arg_keys[5], 71), 0)
    deltas = gaussian(arg_keys[1], (LAYERS, TOKENS, D), 0.5, 6.0, ((0, 8), (2, 16)))
    norm_gain = jnp.clip(1.0 + 0.15 * jax.random.normal(arg_keys[2], (D,), jnp.float32), 0.25, 1.75)
    unembed = draw_unembed(jax.random.fold_in(arg_keys[5], 71), 0)
    targets = with_ends(wide_ids(arg_keys[4], (TOKENS,), VOCAB, 2), jax.random.fold_in(arg_keys[4], 3), 0, VOCAB - 1).astype(jnp.int32)
    return dict(stream_in=stream_in, deltas=deltas, norm_gain=norm_gain, unembed=unembed, targets=targets)


EPSILON = 1e-06

def reference(stream_in, deltas, norm_gain, unembed, targets):
    residual = stream_in.astype(jnp.float32)[None] + jnp.cumsum(deltas.astype(jnp.float32), axis=0)
    mean_square = lax.optimization_barrier(jnp.mean(residual * residual, axis=2, keepdims=True))
    normed = (residual * lax.rsqrt(mean_square + EPSILON) * norm_gain).astype(jnp.bfloat16)
    word_ids = jnp.arange(VOCAB, dtype=jnp.int32)
    hit_mask = word_ids[:, None] == targets.astype(jnp.int32)[None, :]

    def per_layer(layer_rows):
        logits = jnp.dot(unembed, layer_rows.T, preferred_element_type=jnp.float32)
        highest = lax.optimization_barrier(jnp.max(logits, axis=0))
        weights = jnp.exp(logits - highest[None, :])
        masses = lax.optimization_barrier(jnp.sum(weights, axis=0))
        lens_lse = highest + jnp.log(masses)
        moments = lax.optimization_barrier(jnp.sum(weights * logits, axis=0))
        entropy = lens_lse - moments / masses
        picked = lax.optimization_barrier(jnp.sum(jnp.where(hit_mask, logits, jnp.float32(0.0)), axis=0))
        return (lens_lse, entropy, picked - lens_lse)
    lens_lse, lens_entropy, lens_logprob = lax.map(per_layer, normed)
    return (lens_lse, lens_entropy, lens_logprob)
```

```python
import functools

import jax
import jax.numpy as jnp
from jax import lax
from jax.experimental import pallas as pl
from jax.experimental.pallas import tpu as pltpu
from jax.sharding import Mesh
from jax.sharding import PartitionSpec as P

MESH = pl.DeviceIdType.MESH
F32 = jnp.float32
BF16 = jnp.bfloat16
EPSILON = 1e-06

VOCAB = ("vocab_0", "vocab_1")
SECTION_VOCAB = ("section", "vocab_0", "vocab_1")

LINKS = ((0, 1), (0, -1), (1, 1), (1, -1), (2, 1), (2, -1))
TREE = (
    (-1, 0, 0, 1), (0, -1, 0, 3), (0, 0, -1, 5), (0, 0, 1, 4), (0, 1, 0, 2), (1, 0, 0, 0),
    (-1, -1, 0, 1), (0, -1, -1, 3), (0, 0, 2, 4), (0, 1, -1, 5), (2, 0, 0, 0), (-1, 0, -1, 5),
    (0, 1, 1, 4), (0, 2, 0, 3), (1, 0, 1, 0), (-1, 0, 1, 1), (0, -1, 1, 4), (1, -1, 0, 3),
    (1, 1, 0, 0), (-1, 1, 0, 1), (0, 1, 2, 2), (0, -1, 2, 5), (1, 1, -1, 0), (2, -1, 0, 1),
    (-1, 1, -1, 2), (-1, 2, 0, 3), (0, 2, 1, 4), (1, 0, 2, 0), (2, 0, -1, 5), (1, 1, 1, 2),
    (-1, 1, 1, 1), (0, 2, -1, 5), (1, -1, 1, 4), (2, 0, 1, 0), (1, 2, 0, 2), (-1, -1, -1, 1),
    (-1, -1, 1, 4), (1, -1, -1, 5), (1, 0, -1, 0), (1, 2, -1, 2), (-1, -1, 2, 1), (0, 2, 2, 3),
    (1, 1, 2, 5), (2, -1, 1, 4), (2, 1, -1, 0), (-1, 2, -1, 2), (-1, 2, 1, 1), (1, 2, 1, 0),
    (2, -1, -1, 3), (2, 1, 0, 2), (-1, 0, 2, 1), (1, -1, 2, 3), (2, 0, 2, 4), (2, 1, 1, 2),
    (-1, 1, 2, 4), (2, 2, 0, 3), (1, 2, 2, 2), (2, 1, 2, 5), (2, 2, 1, 3), (-1, 2, 2, 3),
    (2, -1, 2, 5), (2, 2, -1, 1), (2, 2, 2, 4),
)
PLAN = (
    (
        (
            (1, 0, 0), (1, 0, 1), (1, 1, 0), (1, 1, 1), (1, 2, 0), (1, 2, 1), (1, 3, 0), (1, 3, 1), (1, 4, 0),
            (1, 4, 1), (1, 5, 0), (1, 5, 1), (1, 0, 2), (1, 1, 2), (1, 2, 2), (1, 3, 2), (1, 4, 2), (1, 5, 2),
            (1, 0, 3), (1, 1, 3), (1, 2, 3), (1, 3, 3), (1, 4, 3), (1, 5, 3), (0, 0, 0), (0, 1, 0), (0, 2, 0),
            (0, 3, 0), (0, 4, 0), (0, 5, 0), (1, 6, 0), (1, 7, 0), (1, 8, 0), (1, 9, 0), (1, 10, 0), (1, 11, 0),
            (1, 12, 0), (1, 13, 0), (1, 14, 0), (1, 15, 0), (1, 16, 0), (1, 17, 0), (1, 18, 0), (0, 0, 1), (0, 1, 1),
            (0, 2, 1), (0, 3, 1), (0, 4, 1), (0, 5, 1), (1, 6, 1), (1, 9, 1), (1, 7, 1), (1, 8, 1), (1, 10, 1),
            (1, 11, 1), (1, 19, 0), (0, 0, 2), (0, 1, 2), (0, 2, 2), (0, 3, 2), (0, 4, 2), (0, 5, 2), (1, 12, 1),
            (1, 13, 1), (0, 0, 3), (0, 1, 3), (0, 2, 3), (0, 3, 3), (0, 4, 3), (0, 5, 3), (0, 6, 0), (0, 7, 0),
            (0, 8, 0), (0, 9, 0), (0, 10, 0), (1, 20, 0), (1, 21, 0), (1, 22, 0), (1, 23, 0), (1, 25, 0), (1, 27, 0),
            (1, 28, 0), (1, 17, 1), (0, 6, 1), (0, 11, 0), (0, 12, 0), (0, 13, 0), (0, 14, 0), (1, 23, 1), (1, 24, 0),
            (1, 26, 0), (1, 29, 0), (1, 30, 0), (1, 31, 0), (1, 33, 0), (1, 7, 2), (1, 35, 0), (1, 36, 0), (1, 38, 0),
            (0, 9, 1), (0, 15, 0), (0, 16, 0), (0, 17, 0), (0, 18, 0), (1, 32, 0), (1, 34, 0), (1, 37, 0), (0, 7, 1),
            (0, 8, 1), (0, 10, 1), (0, 11, 1), (0, 19, 0), (0, 20, 0), (1, 21, 1), (0, 12, 1), (0, 13, 1), (0, 21, 0),
            (0, 22, 0), (0, 23, 0), (1, 39, 0), (1, 40, 0), (1, 41, 0), (1, 42, 0), (1, 43, 0), (1, 44, 0), (1, 49, 0),
            (0, 24, 0), (1, 45, 0), (1, 14, 1), (1, 28, 1), (1, 50, 0), (0, 23, 1), (0, 25, 0), (0, 26, 0), (0, 27, 0),
            (0, 28, 0), (1, 43, 1), (1, 46, 0), (1, 47, 0), (1, 48, 0), (1, 51, 0), (0, 29, 0), (1, 6, 2), (1, 9, 2),
            (1, 22, 1), (1, 55, 0), (0, 17, 1), (0, 30, 0), (0, 31, 0), (0, 32, 0), (0, 33, 0), (1, 52, 0), (1, 53, 0),
            (1, 54, 0), (0, 34, 0), (1, 18, 1), (1, 26, 1), (1, 30, 1), (0, 7, 2), (0, 35, 0), (0, 36, 0), (0, 37, 0),
            (0, 38, 0), (1, 24, 1), (0, 39, 0), (1, 16, 1), (1, 27, 1), (0, 40, 0), (0, 41, 0), (0, 42, 0), (0, 43, 0),
            (0, 44, 0),
        ),
        (
            (1, 56, 0), (1, 57, 0), (1, 58, 0), (1, 59, 0), (1, 20, 1), (0, 45, 0), (1, 61, 0), (1, 11, 2), (1, 32, 1),
            (0, 21, 1), (0, 43, 1), (0, 46, 0), (0, 47, 0), (0, 48, 0), (1, 40, 1), (1, 60, 0),
        ),
        (
            (0, 49, 0), (1, 8, 2), (1, 58, 1), (0, 14, 1), (0, 28, 1), (0, 50, 0), (0, 51, 0), (0, 52, 0), (1, 33, 1),
            (1, 48, 1), (1, 29, 1),
        ),
    ),
    (
        (
            (0, 53, 0), (1, 10, 2), (1, 31, 1), (1, 41, 1), (0, 6, 2), (0, 9, 2), (0, 22, 1), (0, 54, 0), (0, 55, 0),
            (1, 23, 2), (1, 39, 1), (1, 42, 1), (1, 44, 1), (0, 56, 0),
        ),
        (
            (1, 12, 2), (1, 35, 1), (1, 37, 1), (0, 18, 1), (0, 26, 1), (0, 30, 1), (0, 57, 0), (0, 58, 0), (1, 46, 1),
            (1, 47, 1), (1, 62, 0), (1, 34, 1), (0, 24, 1), (1, 45, 1), (1, 15, 1), (1, 38, 1), (1, 55, 1),
        ),
        (
            (0, 16, 1), (0, 27, 1), (0, 59, 0), (0, 60, 0), (0, 61, 0), (1, 51, 1), (0, 20, 1), (1, 13, 2), (1, 14, 2),
            (1, 19, 1), (0, 11, 2), (0, 32, 1), (0, 33, 1), (0, 40, 1), (0, 48, 1),
        ),
    ),
    (
        (),
        (
            (1, 52, 1), (1, 60, 1), (1, 49, 1), (0, 39, 1), (1, 21, 2), (1, 22, 2), (1, 25, 1), (1, 50, 1), (0, 8, 2),
            (0, 23, 2), (0, 42, 1), (0, 44, 1), (0, 58, 1), (1, 43, 2), (1, 56, 1), (1, 57, 1), (1, 62, 1), (1, 53, 1),
        ),
        (
            (0, 29, 1), (1, 18, 2), (1, 54, 1), (1, 59, 1), (0, 10, 2), (0, 31, 1), (0, 41, 1), (0, 46, 1), (0, 62, 0),
            (1, 28, 2), (1, 24, 2),
        ),
    ),
    (
        (),
        (
            (0, 45, 1), (1, 61, 1), (1, 6, 3), (1, 9, 3), (1, 17, 2), (1, 27, 2), (1, 36, 1), (0, 12, 2), (0, 35, 1),
            (0, 37, 1), (0, 47, 1), (0, 51, 1), (1, 20, 2), (0, 34, 1), (1, 7, 3), (1, 11, 3), (1, 30, 2),
        ),
        (
            (0, 15, 1), (0, 38, 1), (0, 52, 1), (0, 55, 1), (0, 60, 1), (0, 56, 1), (1, 16, 2),
        ),
    ),
    (
        (
            (0, 13, 2), (0, 14, 2), (0, 19, 1), (0, 57, 1), (0, 62, 1), (1, 26, 2), (1, 33, 2), (1, 29, 2), (0, 49, 1),
            (1, 8, 3), (1, 10, 3), (1, 31, 2), (1, 35, 2),
        ),
        (
            (0, 21, 2), (0, 22, 2), (0, 25, 1), (0, 43, 2), (0, 50, 1), (1, 39, 2), (1, 40, 2), (1, 42, 2), (1, 44, 2),
            (1, 58, 2), (0, 53, 1), (1, 38, 2), (1, 41, 2), (0, 18, 2), (0, 28, 2), (0, 54, 1), (0, 59, 1), (0, 61, 1),
            (1, 48, 2),
        ),
        (
            (1, 34, 2), (0, 24, 2), (1, 45, 2), (0, 6, 3), (0, 9, 3), (0, 17, 2), (0, 27, 2), (0, 36, 1), (1, 23, 3),
            (1, 32, 2), (1, 37, 2), (1, 51, 2),
        ),
    ),
    (
        (),
        (
            (0, 20, 2), (1, 14, 3), (1, 15, 2), (1, 55, 2), (0, 7, 3), (0, 11, 3), (0, 26, 2), (0, 30, 2), (0, 33, 2),
            (1, 21, 3), (1, 46, 2), (1, 47, 2), (1, 52, 2), (1, 49, 2), (0, 39, 2),
        ),
        (
            (1, 12, 3), (1, 13, 3), (1, 19, 2), (1, 22, 3), (0, 16, 2), (0, 40, 2), (0, 42, 2), (0, 44, 2), (0, 58, 2),
            (1, 56, 2), (1, 57, 2), (1, 62, 2), (1, 53, 2), (0, 29, 2),
        ),
    ),
    (
        (),
        (
            (1, 18, 3), (1, 25, 2), (0, 8, 3), (0, 10, 3), (0, 31, 2), (0, 35, 2), (0, 48, 2), (1, 28, 3), (1, 60, 2),
            (1, 24, 3), (0, 45, 2), (1, 61, 2), (1, 27, 3), (1, 50, 2), (1, 54, 2), (1, 59, 2), (0, 23, 3), (0, 32, 2),
            (0, 37, 2), (0, 38, 2), (0, 41, 2), (1, 43, 3),
        ),
        (
            (1, 20, 3), (0, 34, 2), (1, 17, 3), (1, 36, 2), (0, 21, 3), (0, 46, 2), (0, 47, 2), (0, 51, 2), (0, 52, 2),
            (1, 40, 3),
        ),
    ),
    (
        (),
        (
            (0, 56, 2), (1, 41, 3), (0, 14, 3), (0, 15, 2), (0, 55, 2), (0, 57, 2), (0, 62, 2), (1, 33, 3), (1, 29, 3),
        ),
        (
            (0, 49, 2), (1, 16, 3), (1, 35, 3), (1, 38, 3), (0, 12, 3), (0, 13, 3), (0, 19, 2), (0, 22, 3), (0, 60, 2),
            (1, 26, 3), (1, 30, 3), (1, 31, 3), (1, 39, 3), (1, 42, 3), (1, 44, 3),
        ),
    ),
    (
        (
            (0, 53, 2), (1, 15, 3), (1, 36, 3), (0, 18, 3), (0, 25, 2), (0, 28, 3), (0, 43, 3), (0, 61, 2), (1, 48, 3),
            (1, 58, 3), (1, 34, 3),
        ),
        (
            (0, 24, 3), (1, 45, 3), (1, 19, 3), (0, 27, 3), (0, 50, 2), (0, 54, 2), (0, 59, 2), (1, 51, 3), (0, 20, 3),
            (1, 55, 3),
        ),
        (
            (0, 17, 3), (0, 33, 3), (0, 36, 2), (0, 40, 3), (1, 32, 3), (1, 37, 3), (1, 52, 3), (1, 49, 3), (0, 39, 3),
            (0, 42, 3), (1, 56, 3), (1, 25, 3), (1, 50, 3),
        ),
    ),
    (
        (),
        (
            (0, 26, 3), (0, 30, 3), (0, 41, 3), (0, 44, 3), (1, 46, 3), (1, 47, 3), (1, 54, 3), (1, 57, 3), (1, 53, 3),
            (0, 29, 3), (0, 31, 3), (1, 59, 3), (0, 16, 3), (0, 35, 3), (0, 38, 3), (0, 48, 3), (1, 60, 3),
        ),
        (
            (0, 45, 3), (1, 61, 3), (0, 15, 3), (0, 36, 3), (0, 58, 3), (1, 62, 3),
        ),
    ),
    (
        (),
        (
            (0, 34, 3), (0, 37, 3), (0, 19, 3), (0, 32, 3), (0, 51, 3), (0, 47, 3), (0, 56, 3), (0, 57, 3),
        ),
        (
            (0, 46, 3), (0, 52, 3), (0, 55, 3), (0, 49, 3), (0, 60, 3),
        ),
    ),
    (
        (),
        (
            (0, 25, 3), (0, 50, 3), (0, 54, 3), (0, 53, 3), (0, 59, 3), (0, 61, 3), (0, 62, 3),
        ),
        (),
    ),
    (
        (),
        (),
        (),
    ),
    (
        (),
        (),
        (),
    ),
    (
        (),
        (),
        (),
    ),
    (
        (),
        (),
        (),
    ),
)
PLANES = (0, 1, -1, 2)

GROUPS = 4
GTOK = 16
FILL = -1e30


def pick(index, values):
    out = values[-1]
    for k in range(len(values) - 2, -1, -1):
        out = jnp.where(index == k, values[k], out)
    return out


def dispatch(index, branches, low=0, high=None):
    high = len(branches) if high is None else high
    if not any(branches[low:high]):
        return
    if high - low == 1:
        branches[low]()
        return
    mid = (low + high) // 2

    @pl.when(index < mid)
    def _():
        dispatch(index, branches, low, mid)

    @pl.when(index >= mid)
    def _():
        dispatch(index, branches, mid, high)


def kernel(
    stream_hbm, deltas_hbm, gain_hbm, unembed_hbm, targets_hbm, out_ref,
    stream_v, deltas_v, targets_v, gains, outbox, gat, words, rows, acc, squares,
    stats, from_x, stats_x, from_y, stats_y, from_z,
    load_sem, own_sem, words_send, words_recv, gain_send, gain_recv,
    part_send, part_recv, send_sem, recv_sem,
    x_send, x_recv, y_send, y_recv, z_send, z_recv,
):
    section = lax.axis_index("section")
    x = lax.axis_index("vocab_0")
    z = lax.axis_index("vocab_1")
    y = section // 2
    core = section % 2
    sign = 1 - 2 * core
    nwords = unembed_hbm.shape[0]
    plane_width = unembed_hbm.shape[1] // 4
    home = (x, y, z)

    def device(xx, yy, zz, cc):
        return (yy * 2 + cc, xx, zz)

    def moved(axis, step):
        at = list(home)
        at[axis] = lax.rem(at[axis] + step + 4, 4)
        return tuple(at)

    neighbours = [device(*moved(axis, way * sign), core) for axis, way in LINKS]
    partner = device(x, y, z, 1 - core)
    source = [{d: lax.rem(home[axis] - sign * d + 4, 4) for d in (-1, 0, 1, 2)} for axis in range(3)]

    loads = [
        pltpu.make_async_copy(stream_hbm, stream_v, load_sem.at[0]),
        pltpu.make_async_copy(deltas_hbm, deltas_v, load_sem.at[1]),
        pltpu.make_async_copy(targets_hbm, targets_v, load_sem.at[2]),
        pltpu.make_async_copy(gain_hbm, gains.at[x * 4 + z], load_sem.at[3]),
    ]
    for copy in loads:
        copy.start()

    barrier = pltpu.get_barrier_semaphore()
    for axis in range(3):
        for step in (1, 2, 3):
            at = moved(axis, step)
            pl.semaphore_signal(barrier, inc=1, device_id=device(*at, core), device_id_type=MESH)
            if axis == 2:
                pl.semaphore_signal(barrier, inc=1, device_id=device(*at, 1 - core), device_id_type=MESH)
    pl.semaphore_signal(barrier, inc=1, device_id=partner, device_id_type=MESH)

    def columns(plane):
        return pl.ds(pl.multiple_of(plane * plane_width, 128), plane_width)

    own_words = []
    for p, dx in enumerate(PLANES):
        plane = source[0][dx]
        own_words.append(
            pltpu.make_async_copy(
                unembed_hbm.at[:, columns(plane)], words.at[0, plane, pl.ds(0, nwords)], own_sem.at[p]
            )
        )
        own_words[-1].start()

    for copy in loads:
        copy.wait()

    lane = lax.broadcasted_iota(jnp.int32, (GTOK, 128), 1)
    low = lane < 64
    odd = lax.rem(z, 2) == 1
    first = jnp.where(section == 0, 1.0, 0.0).astype(F32)
    my_slot = ((x * 4 + y) * 4 + z) * GROUPS
    for half in range(2):
        for g in range(GROUPS):
            t0 = half * 64 + g * GTOK
            tiles = []
            for k in range(3):
                cols = slice(128 * k, min(128 * k + 128, 320))
                base = stream_v[t0 : t0 + GTOK, cols].astype(F32)
                former = deltas_v[0, t0 : t0 + GTOK, cols].astype(F32) + base * first
                kept = former.astype(BF16).astype(F32)
                latter = deltas_v[1, t0 : t0 + GTOK, cols].astype(F32) + (former - kept)
                pair = [kept, latter]
                if k == 2:
                    pair = [jnp.concatenate([v, jnp.zeros_like(v)], axis=1) for v in pair]
                tiles.append(pair)
            packed = []
            heads = []
            for l in range(2):
                a0, a1, a2 = (tiles[k][l] for k in range(3))
                r0, r1, r2 = (pltpu.roll(v, 64, 1) for v in (a0, a1, a2))
                packed.append(jnp.where(odd, jnp.where(low, r0, r1), a0))
                packed.append(jnp.where(odd, jnp.where(low, r1, r2), a1))
                heads.append(jnp.where(odd, a0, a2))
            lead = jnp.where(odd, heads[1], heads[0])
            trail = jnp.where(odd, heads[0], heads[1])
            packed.append(jnp.where(low, lead, pltpu.roll(trail, 64, 1)))

            @pl.when(core == half)
            def _():
                for k, value in enumerate(packed):
                    gat[my_slot + g, core, k] = value.astype(BF16)

            @pl.when(core != half)
            def _():
                for k, value in enumerate(packed):
                    outbox[g, k] = value.astype(BF16)

    acc[:, 1184:1200, :] = jnp.full((2, 16, 256), FILL, F32)

    pl.semaphore_wait(barrier, 13)

    part = pltpu.make_async_remote_copy(
        src_ref=outbox,
        dst_ref=gat.at[pl.ds(my_slot, GROUPS), core],
        send_sem=part_send,
        recv_sem=part_recv,
        device_id=partner,
        device_id_type=MESH,
    )
    part.start()

    def gain_copy(n, link):
        at = (source[0][n[0]] * 4 + source[2][n[2]])
        place = (TREE_INDEX[child(n, link)] if link is not None else TREE_INDEX[n])
        return pltpu.make_async_remote_copy(
            src_ref=gains.at[at],
            dst_ref=gains.at[at],
            send_sem=gain_send.at[GAIN_INDEX[place]],
            recv_sem=gain_recv.at[GAIN_INDEX[place]],
            device_id=neighbours[link or 0],
            device_id_type=MESH,
        )

    def block_copy(n, row, link, g):
        slot = source[0][n[0]] * 64 + source[1][n[1]] * 16 + source[2][n[2]] * 4 + g
        return pltpu.make_async_remote_copy(
            src_ref=gat.at[slot],
            dst_ref=gat.at[slot],
            send_sem=send_sem.at[g],
            recv_sem=recv_sem.at[row * GROUPS + g],
            device_id=neighbours[link],
            device_id_type=MESH,
        )

    def send_gain(n):
        for row, (dx, dy, dz, link) in enumerate(TREE):
            if dy == 0 and parent((dx, dy, dz), link) == n:
                gain_copy(n, link).start()

    def run(actions):
        for kind, row, g in actions:
            dx, dy, dz, link = TREE[row]
            n = (dx, dy, dz)
            if kind == 0:
                block_copy(n, row, link, g).wait_recv()
                if g == 0 and dy == 0:
                    gain_copy(n, None).wait_recv()
                    send_gain(n)
            else:
                block_copy(parent(n, link), row, link, g).start()

    send_gain((0, 0, 0))

    their_words = []
    for p, dx in enumerate(PLANES):
        plane = lax.rem(x + sign * dx + 4, 4)
        their_words.append(
            pltpu.make_async_remote_copy(
                src_ref=unembed_hbm.at[:, columns(plane)],
                dst_ref=words.at[1, plane, pl.ds(0, nwords)],
                send_sem=words_send.at[p],
                recv_sem=words_recv.at[p],
                device_id=partner,
                device_id_type=MESH,
            )
        )

    part.wait_recv()
    their_words[0].start()
    their_words[1].start()
    their_words[2].start()
    their_words[3].start()

    def body(s, carry):
        g = s // 4
        p = lax.rem(s, 4)
        plane = pick(p, [source[0][dx] for dx in PLANES])
        dispatch(s, [functools.partial(run, step[0]) if step[0] else None for step in PLAN])

        running = [jnp.zeros((GTOK, 128), F32) for _ in range(10)]
        gain_rows = []
        for zp in range(2):
            both = gains[plane * 4 + 2 * zp] + gains[plane * 4 + 2 * zp + 1]
            gain_rows.extend(jnp.broadcast_to(both[k : k + 1, :], (GTOK, 128)) for k in range(5))
        for yy in range(4):
            for cc in range(2):
                blocks = []
                for zz in range(4):
                    slot = plane * 64 + yy * 16 + zz * 4 + g
                    blocks.append(slot)
                for l in range(2):
                    layer = 4 * yy + 2 * cc + l
                    total = jnp.zeros((GTOK, 128), F32)
                    for zp in range(2):
                        even, other = blocks[2 * zp], blocks[2 * zp + 1]
                        pe = gat[even, cc, 4].astype(F32)
                        po = gat[other, cc, 4].astype(F32)
                        if l == 0:
                            middle = jnp.where(low, pe, po)
                        else:
                            middle = pltpu.roll(jnp.where(low, po, pe), 64, 1)
                        values = [
                            gat[even, cc, 2 * l].astype(F32),
                            gat[even, cc, 2 * l + 1].astype(F32),
                            middle,
                            gat[other, cc, 2 * l].astype(F32),
                            gat[other, cc, 2 * l + 1].astype(F32),
                        ]
                        for k in range(5):
                            at = 5 * zp + k
                            running[at] = running[at] + values[k]
                            total = total + running[at] * running[at]
                            rows[layer * GTOK : (layer + 1) * GTOK, at * 128 : (at + 1) * 128] = (
                                running[at] * gain_rows[at]
                            ).astype(BF16)
                    former = squares[layer * GTOK : (layer + 1) * GTOK, :]
                    squares[layer * GTOK : (layer + 1) * GTOK, :] = jnp.where(p == 0, 0.0, former) + total

        @pl.when(s < 4)
        def _():
            pltpu.make_async_copy(
                unembed_hbm.at[:, columns(plane)], words.at[0, plane, pl.ds(0, nwords)], own_sem.at[p]
            ).wait()
            pltpu.make_async_remote_copy(
                src_ref=unembed_hbm.at[:, columns(plane)],
                dst_ref=words.at[1, plane, pl.ds(0, nwords)],
                send_sem=words_send.at[p],
                recv_sem=words_recv.at[p],
                device_id=partner,
                device_id_type=MESH,
            ).wait_recv()

        for half in range(2):
            product = lax.dot_general(
                words[half, plane, 0:nwords, :], rows[...], (((1,), (1,)), ((), ())), preferred_element_type=F32
            )
            acc[half, 0:nwords, :] = jnp.where(p == 0, 0.0, acc[half, 0:nwords, :]) + product
            dispatch(s, [functools.partial(run, step[1 + half]) if step[1 + half] else None for step in PLAN])

        @pl.when(p == 3)
        def _():
            sums = jnp.sum(jnp.transpose(squares[...]), axis=0, keepdims=True)
            inverse = lax.rsqrt(sums / (4 * plane_width) + EPSILON)

            def top(i, most):
                start = pl.multiple_of(i * 200, 8)
                for half in range(2):
                    for k in range(25):
                        most = jnp.maximum(most, acc[half, pl.ds(start + 8 * k, 8), :])
                return most

            most = lax.fori_loop(0, 6, top, jnp.full((8, 256), FILL, F32))
            scale = jnp.broadcast_to(inverse, (8, 256))
            peak = jnp.max(most, axis=0, keepdims=True) * inverse
            peaks = jnp.broadcast_to(peak, (8, 256))
            target = targets_v[core * GROUPS + g]
            sublane = lax.broadcasted_iota(jnp.int32, (8, 256), 0)
            wanted = []
            for half in range(2):
                holder = core if half == 0 else 1 - core
                first_word = (((y * 2 + holder) * 4 + x) * 4 + z) * nwords
                local = target - first_word
                local = jnp.where(local < nwords, local, -8)
                wanted.append(jnp.broadcast_to(local, (8, 256)) - sublane)

            def fold(i, carry):
                mass, moment, picked = carry
                start = pl.multiple_of(i * 200, 8)
                for half in range(2):
                    for k in range(25):
                        z_all = acc[half, pl.ds(start + 8 * k, 8), :] * scale
                        z_rel = z_all - peaks
                        e = jnp.exp(z_rel)
                        mass = mass + e
                        moment = moment + e * z_rel
                        picked = jnp.where(wanted[half] == start + 8 * k, z_all, picked)
                return mass, moment, picked

            zero = jnp.zeros((8, 256), F32)
            mass, moment, picked = lax.fori_loop(0, 6, fold, (zero, zero, zero))
            found = [peak] + [jnp.sum(v, axis=0, keepdims=True) for v in (mass, moment, picked)]
            for k, value in enumerate(found):
                stats[g, 2 * k : 2 * k + 1, :] = value[:, 0:128]
                stats[g, 2 * k + 1 : 2 * k + 2, :] = value[:, 128:256]

        return carry

    lax.fori_loop(0, 4 * GROUPS, body, 0)

    def joined(parts):
        tops = [part[:, 0:2, :] for part in parts]
        most = functools.reduce(jnp.maximum, tops)
        shifts = [top - most for top in tops]
        factors = [jnp.exp(shift) for shift in shifts]
        mass = sum(f * part[:, 2:4, :] for f, part in zip(factors, parts))
        moment = sum(
            f * (part[:, 4:6, :] + shift * part[:, 2:4, :]) for f, shift, part in zip(factors, shifts, parts)
        )
        picked = sum(part[:, 6:8, :] for part in parts)
        return most, mass, moment, picked

    waits = []

    def exchanged(axis, mine, inbox, send, recv, result):
        copies = []
        for step in (1, 2, 3):
            copies.append(
                pltpu.make_async_remote_copy(
                    src_ref=mine,
                    dst_ref=inbox.at[step - 1],
                    send_sem=send.at[step - 1],
                    recv_sem=recv.at[step - 1],
                    device_id=device(*moved(axis, step), core),
                    device_id_type=MESH,
                )
            )
        for copy in copies:
            copy.start()
        for copy in copies:
            copy.wait_recv()
        waits.extend(copies)
        for k, value in enumerate(joined([mine[...]] + [inbox[k] for k in range(3)])):
            result[:, 2 * k : 2 * k + 2, :] = value

    exchanged(0, stats, from_x, x_send, x_recv, stats_x)
    exchanged(1, stats_x, from_y, y_send, y_recv, stats_y)

    def last_copy(step, other, towards):
        cc = 1 - core if other else core
        origin = core if towards else cc
        return pltpu.make_async_remote_copy(
            src_ref=stats_y,
            dst_ref=from_z.at[origin, step],
            send_sem=z_send.at[4 * other + step],
            recv_sem=z_recv.at[4 * other + step],
            device_id=device(*moved(2, step), cc),
            device_id_type=MESH,
        )

    lasts = [(1, True), (2, True), (3, True), (1, False), (2, False), (3, False), (0, True)]
    for step, other in lasts:
        last_copy(step, other, True).start()
    from_z[core, 0] = stats_y[...]
    for step, other in lasts:
        last_copy(step, other, False).wait_recv()
    for half in range(2):
        most, mass, moment, picked = joined([from_z[half, k] for k in range(4)])
        log_mass = jnp.log(mass)
        lse = most + log_mass
        out_ref[0, half] = lse
        out_ref[1, half] = log_mass - moment / mass
        out_ref[2, half] = picked - lse

    for step, other in lasts:
        last_copy(step, other, True).wait_send()
    for copy in waits:
        copy.wait_send()
    part.wait_send()
    for copy in their_words:
        copy.wait_send()
    for row, (dx, dy, dz, link) in enumerate(TREE):
        if dy == 0:
            gain_copy(parent((dx, dy, dz), link), link).wait_send()
    for g in range(GROUPS):
        pltpu.make_async_remote_copy(
            src_ref=gat.at[pl.ds(0, len(TREE))],
            dst_ref=gat.at[pl.ds(0, len(TREE))],
            send_sem=send_sem.at[g],
            recv_sem=recv_sem.at[0],
            device_id=neighbours[0],
            device_id_type=MESH,
        ).wait_send()


def wrapped(c):
    return (c + 1) % 4 - 1


def parent(n, link):
    axis, way = LINKS[link]
    n = list(n)
    n[axis] = wrapped(n[axis] - way)
    return tuple(n)


def child(n, link):
    axis, way = LINKS[link]
    n = list(n)
    n[axis] = wrapped(n[axis] + way)
    return tuple(n)


TREE_INDEX = {row[:3]: k for k, row in enumerate(TREE)}
GAIN_INDEX = {k: i for i, k in enumerate(k for k, row in enumerate(TREE) if row[1] == 0)}


def shards(stream_in, deltas, norm_gain, unembed, targets):
    nwords, width = unembed.shape
    odd = lax.rem(lax.axis_index("vocab_1"), 2) == 1
    gap = jnp.zeros((320,), F32)
    rest = jnp.zeros((384,), F32)
    gain = jnp.where(
        odd, jnp.concatenate([gap, norm_gain, rest]), jnp.concatenate([norm_gain, gap, rest])
    ).reshape(8, 128)
    wanted = jnp.broadcast_to(targets.reshape(8, 1, 1, GTOK), (8, 1, 16, GTOK)).reshape(8, 1, 256)
    anywhere = pl.BlockSpec(memory_space=pl.ANY)
    dma = pltpu.SemaphoreType.DMA
    out = pl.pallas_call(
        kernel,
        out_shape=jax.ShapeDtypeStruct((3, 2, GROUPS, 2, 128), F32),
        in_specs=[anywhere] * 5,
        out_specs=pl.BlockSpec(memory_space=pltpu.VMEM),
        scratch_shapes=[
            pltpu.VMEM((128, 320), BF16),
            pltpu.VMEM((2, 128, 320), BF16),
            pltpu.VMEM((8, 1, 256), jnp.int32),
            pltpu.VMEM((16, 8, 128), F32),
            pltpu.VMEM((GROUPS, 5, GTOK, 128), BF16),
            pltpu.VMEM((64 * GROUPS, 2, 5, GTOK, 128), BF16),
            pltpu.VMEM((2, 4, nwords, width // 4), BF16),
            pltpu.VMEM((256, width // 4), BF16),
            pltpu.VMEM((2, 1200, 256), F32),
            pltpu.VMEM((256, 128), F32),
            pltpu.VMEM((GROUPS, 8, 128), F32),
            pltpu.VMEM((3, GROUPS, 8, 128), F32),
            pltpu.VMEM((GROUPS, 8, 128), F32),
            pltpu.VMEM((3, GROUPS, 8, 128), F32),
            pltpu.VMEM((GROUPS, 8, 128), F32),
            pltpu.VMEM((2, 4, GROUPS, 8, 128), F32),
            dma((4,)),
            dma((4,)),
            dma((4,)),
            dma((4,)),
            dma((15,)),
            dma((15,)),
            dma,
            dma,
            dma((GROUPS,)),
            dma((63 * GROUPS,)),
            dma((3,)),
            dma((3,)),
            dma((3,)),
            dma((3,)),
            dma((8,)),
            dma((8,)),
        ],
        compiler_params=pltpu.CompilerParams(
            collective_id=0, has_side_effects=True, vmem_limit_bytes=60 * 1024 * 1024
        ),
    )(stream_in, deltas, gain, unembed, wanted)
    layers = out.reshape(3, 2, GROUPS, 16, GTOK).transpose(0, 3, 1, 2, 4).reshape(3, 16, 128)
    mine = lax.dynamic_slice_in_dim(layers, 2 * lax.axis_index("section"), 2, axis=1)
    return mine[0], mine[1], mine[2]


def solution(mesh):
    torus = Mesh(
        mesh.devices.reshape(mesh.shape["section"], 4, 4), ("section", "vocab_0", "vocab_1")
    )
    placed = (P(None, VOCAB), P("section", None, VOCAB), P(VOCAB), P(SECTION_VOCAB, None), P())
    return jax.shard_map(
        shards,
        mesh=torus,
        in_specs=placed,
        out_specs=(P("section", None), P("section", None), P("section", None)),
        check_vma=False,
    )
```

```python
import functools

import jax
import jax.numpy as jnp
from jax import lax
from jax.experimental import pallas as pl
from jax.experimental.pallas import tpu as pltpu
from jax.sharding import Mesh
from jax.sharding import PartitionSpec as P

MESH = pl.DeviceIdType.MESH
F32 = jnp.float32
BF16 = jnp.bfloat16
EPSILON = 1e-06

VOCAB = ("vocab_0", "vocab_1")
SECTION_VOCAB = ("section", "vocab_0", "vocab_1")

LINKS = ((0, 1), (0, -1), (1, 1), (1, -1), (2, 1), (2, -1))
TREE = (
    (-1, 0, 0, 1), (0, -1, 0, 3), (0, 0, -1, 5), (0, 0, 1, 4), (0, 1, 0, 2), (1, 0, 0, 0),
    (-1, -1, 0, 1), (-1, 0, -1, 1), (-1, 0, 1, 1), (-1, 1, 0, 1), (0, -1, -1, 3), (0, -1, 1, 3),
    (0, 0, 2, 5), (0, 1, -1, 5), (0, 1, 1, 4), (0, 2, 0, 2), (1, -1, 0, 0), (1, 0, -1, 0),
    (1, 0, 1, 0), (1, 1, 0, 0), (2, 0, 0, 1), (-1, -1, -1, 5), (-1, -1, 1, 3), (-1, 0, 2, 4),
    (-1, 1, -1, 1), (-1, 1, 1, 1), (-1, 2, 0, 3), (0, -1, 2, 4), (0, 1, 2, 4), (0, 2, -1, 3),
    (0, 2, 1, 2), (1, -1, -1, 5), (1, -1, 1, 3), (1, 0, 2, 5), (1, 1, -1, 5), (1, 1, 1, 4),
    (1, 2, 0, 3), (2, -1, 0, 0), (2, 0, -1, 0), (2, 0, 1, 0), (2, 1, 0, 1), (-1, -1, 2, 5),
    (-1, 1, 2, 2), (-1, 2, -1, 2), (-1, 2, 1, 3), (0, 2, 2, 2), (1, -1, 2, 0), (1, 1, 2, 5),
    (1, 2, -1, 5), (1, 2, 1, 2), (2, -1, -1, 3), (2, -1, 1, 0), (2, 0, 2, 1), (2, 1, -1, 5),
    (2, 1, 1, 1), (2, 2, 0, 2), (-1, 2, 2, 2), (1, 2, 2, 4), (2, -1, 2, 3), (2, 1, 2, 2),
    (2, 2, -1, 2), (2, 2, 1, 0), (2, 2, 2, 4),
)
PLAN = (
    (
        (1, 0, 0), (1, 1, 0), (1, 2, 0), (1, 3, 0), (1, 4, 0), (1, 5, 0), (1, 0, 1), (1, 1, 1), (1, 2, 1),
        (1, 3, 1), (1, 4, 1), (1, 5, 1), (1, 0, 2), (1, 1, 2), (1, 2, 2), (1, 3, 2), (1, 4, 2), (1, 5, 2),
        (1, 0, 3), (1, 1, 3), (1, 2, 3), (1, 3, 3), (1, 4, 3), (1, 5, 3), (0, 0, 0), (0, 1, 0), (0, 2, 0),
        (0, 3, 0), (0, 4, 0), (0, 5, 0), (1, 9, 0), (1, 11, 0), (1, 13, 0), (1, 14, 0), (1, 15, 0), (1, 19, 0),
        (1, 8, 0), (1, 10, 0), (0, 0, 1), (0, 1, 1), (0, 2, 1), (0, 3, 1), (0, 4, 1), (0, 5, 1), (1, 13, 1),
        (1, 14, 1), (1, 15, 1), (1, 19, 1), (1, 6, 0), (1, 11, 1), (1, 12, 0), (1, 16, 0), (0, 0, 2), (0, 1, 2),
        (0, 2, 2), (0, 3, 2), (0, 4, 2), (0, 5, 2), (1, 14, 2), (1, 15, 2), (1, 9, 1), (1, 10, 1), (1, 13, 2),
        (1, 18, 0), (0, 0, 3), (0, 1, 3), (0, 2, 3), (0, 3, 3), (0, 4, 3), (0, 5, 3), (1, 14, 3), (1, 15, 3),
        (1, 8, 1), (1, 11, 2), (1, 12, 1), (1, 17, 0), (0, 9, 0), (0, 11, 0), (0, 13, 0), (0, 14, 0), (0, 15, 0),
        (0, 19, 0), (1, 30, 0), (1, 35, 0), (1, 10, 2), (1, 34, 0), (1, 19, 2), (1, 40, 0), (0, 8, 0), (0, 10, 0),
        (0, 13, 1), (0, 14, 1), (0, 15, 1), (0, 19, 1), (1, 23, 0), (1, 30, 1), (1, 22, 0), (1, 24, 0), (1, 16, 1),
        (1, 34, 1), (1, 35, 1), (0, 6, 0), (0, 11, 1), (0, 12, 0), (0, 14, 2), (0, 15, 2), (0, 16, 0), (1, 30, 2),
        (1, 21, 0), (1, 25, 0), (1, 18, 1), (1, 36, 0), (1, 27, 0), (0, 9, 1), (0, 10, 1), (0, 13, 2), (0, 14, 3),
        (0, 15, 3), (0, 18, 0), (1, 30, 3), (1, 31, 0), (1, 32, 0), (1, 17, 1), (1, 40, 1), (1, 28, 0), (0, 8, 1),
        (0, 11, 2), (0, 12, 1), (0, 17, 0), (1, 6, 1), (1, 29, 0), (1, 33, 0), (1, 38, 0), (0, 30, 0), (0, 35, 0),
        (1, 49, 0), (1, 23, 1), (0, 10, 2), (0, 34, 0), (0, 19, 2), (0, 40, 0), (1, 26, 0), (1, 19, 3), (1, 53, 0),
        (0, 23, 0), (0, 30, 1), (1, 42, 0), (1, 52, 0), (1, 35, 2), (0, 22, 0), (0, 24, 0), (0, 16, 1), (0, 34, 1),
        (1, 9, 2), (1, 44, 0), (1, 47, 0), (1, 39, 0), (0, 30, 2), (0, 35, 1), (1, 49, 1), (1, 27, 1), (1, 55, 0),
        (0, 21, 0), (0, 25, 0), (0, 18, 1), (0, 36, 0), (1, 41, 0), (1, 8, 2), (1, 36, 1), (0, 27, 0), (0, 30, 3),
        (1, 46, 0), (1, 28, 1), (0, 31, 0), (0, 32, 0), (0, 17, 1), (0, 40, 1), (1, 32, 1), (1, 48, 0), (1, 20, 0),
        (0, 28, 0), (1, 45, 0), (0, 49, 0), (1, 57, 0), (1, 61, 0), (1, 43, 0), (0, 6, 1), (0, 29, 0), (0, 33, 0),
        (0, 38, 0), (1, 7, 0), (1, 50, 0), (1, 51, 0), (1, 53, 1), (0, 23, 1), (0, 42, 0), (1, 56, 0), (0, 26, 0),
        (0, 19, 3), (0, 52, 0), (0, 53, 0), (1, 35, 3), (1, 21, 1), (1, 58, 0), (1, 38, 1), (1, 54, 0), (0, 35, 2),
        (0, 49, 1), (1, 57, 1), (1, 59, 0), (0, 9, 2), (0, 44, 0), (0, 47, 0), (0, 39, 0), (1, 22, 1), (1, 24, 1),
        (1, 31, 1), (1, 37, 0), (0, 27, 1), (0, 55, 0), (1, 60, 0), (0, 41, 0), (0, 8, 2), (0, 46, 0), (0, 36, 1),
        (1, 23, 2), (1, 29, 1), (1, 48, 1), (1, 52, 1), (1, 61, 1), (0, 28, 1), (0, 45, 0),
    ),
    (
        (1, 49, 2), (0, 32, 1), (0, 48, 0), (0, 20, 0), (0, 61, 0), (1, 62, 0), (1, 25, 1), (1, 26, 1), (1, 16, 2),
        (1, 47, 1), (0, 57, 0),
    ),
    (
        (1, 27, 2), (0, 43, 0), (1, 42, 1), (0, 7, 0), (0, 50, 0), (0, 51, 0), (0, 53, 1), (1, 22, 2), (1, 18, 2),
        (1, 33, 1), (1, 40, 2),
    ),
    (
        (0, 35, 3), (1, 28, 2), (0, 56, 0), (1, 45, 1), (0, 21, 1), (0, 58, 0), (0, 38, 1), (0, 54, 0), (1, 6, 2),
        (1, 41, 1), (1, 17, 2), (1, 50, 1),
    ),
    (
        (0, 57, 1), (1, 28, 3), (0, 59, 0), (1, 55, 1), (0, 22, 1), (0, 24, 1), (0, 31, 1), (0, 37, 0), (1, 9, 3),
        (1, 44, 1), (1, 46, 1), (1, 34, 2),
    ),
    (
        (0, 23, 2), (0, 60, 0), (0, 29, 1), (0, 48, 1), (0, 52, 1), (0, 61, 1), (1, 59, 1), (1, 62, 1), (1, 8, 3),
        (1, 13, 3), (1, 51, 1), (1, 58, 1), (0, 62, 0),
    ),
    (
        (0, 49, 2), (1, 57, 2), (1, 43, 1), (0, 25, 1), (0, 26, 1), (0, 16, 2), (0, 47, 1), (1, 31, 2), (1, 36, 2),
        (1, 20, 1), (1, 39, 1),
    ),
    (
        (0, 27, 2), (0, 42, 1), (1, 56, 1), (0, 22, 2), (0, 18, 2), (0, 33, 1), (0, 40, 2), (1, 7, 1), (1, 32, 2),
        (1, 37, 1), (1, 53, 2), (0, 28, 2), (0, 45, 1),
    ),
    (
        (1, 60, 1), (0, 6, 2), (0, 41, 1), (0, 17, 2), (0, 50, 1), (1, 21, 2), (1, 11, 3), (1, 38, 2), (1, 54, 1),
        (0, 28, 3),
    ),
    (
        (0, 55, 1), (1, 49, 3), (0, 9, 3), (0, 44, 1), (0, 46, 1), (0, 34, 2), (1, 24, 2), (1, 44, 2), (1, 12, 2),
        (1, 61, 2), (0, 62, 1),
    ),
    (
        (0, 59, 1), (1, 42, 2), (0, 8, 3), (0, 13, 3), (0, 51, 1), (0, 58, 1), (1, 23, 3), (1, 29, 2), (1, 16, 3),
        (1, 47, 2), (1, 52, 2), (0, 57, 2),
    ),
    (
        (0, 43, 1), (1, 45, 2), (0, 31, 2), (0, 36, 2), (0, 20, 1), (0, 39, 1), (1, 25, 2), (1, 26, 2), (1, 18, 3),
        (1, 48, 2), (0, 56, 1), (1, 55, 2), (0, 7, 1), (0, 32, 2), (0, 37, 1), (0, 53, 2),
    ),
    (
        (1, 10, 3), (1, 17, 3), (1, 33, 2), (1, 40, 3), (0, 60, 1), (1, 60, 2),
    ),
    (
        (0, 21, 2), (0, 11, 3), (0, 38, 2), (0, 54, 1), (1, 27, 3), (1, 6, 3), (1, 41, 2), (1, 46, 2), (1, 50, 2),
        (0, 49, 3),
    ),
    (
        (0, 24, 2), (0, 44, 2), (0, 12, 2), (0, 61, 2), (1, 43, 2), (1, 62, 2), (1, 22, 3), (1, 34, 3), (1, 51, 2),
        (1, 20, 2), (0, 23, 3), (1, 57, 3), (0, 42, 2), (1, 56, 2),
    ),
    (
        (0, 29, 2), (0, 16, 3), (0, 47, 2), (0, 52, 2), (1, 7, 2), (1, 31, 3), (1, 58, 2), (1, 39, 2), (0, 45, 2),
        (1, 59, 2),
    ),
    (
        (0, 25, 2), (0, 26, 2), (0, 18, 3), (0, 48, 2), (1, 12, 3), (1, 36, 3), (1, 37, 2), (1, 54, 2), (0, 55, 2),
        (1, 42, 3),
    ),
    (
        (0, 10, 3), (0, 17, 3), (0, 33, 2), (0, 40, 3), (1, 24, 3), (1, 32, 3), (1, 38, 3), (1, 53, 3), (0, 27, 3),
        (0, 60, 2), (1, 45, 3), (0, 6, 3), (0, 41, 2), (0, 46, 2), (0, 50, 2),
    ),
    (
        (1, 21, 3), (1, 29, 3), (1, 52, 3), (1, 61, 3), (0, 62, 2), (0, 43, 2), (1, 55, 3),
    ),
    (
        (0, 22, 3), (0, 34, 3), (0, 51, 2), (0, 20, 2), (1, 25, 3), (1, 44, 3), (1, 46, 3), (1, 47, 3), (0, 57, 3),
        (0, 56, 2), (0, 7, 2), (0, 31, 3), (0, 58, 2), (0, 39, 2),
    ),
    (
        (1, 26, 3), (1, 33, 3), (1, 20, 3), (1, 39, 3), (0, 59, 2),
    ),
    (
        (0, 12, 3), (0, 36, 3), (0, 37, 2), (0, 54, 2), (1, 7, 3), (1, 48, 3), (1, 37, 3), (0, 42, 3), (1, 56, 3),
    ),
    (
        (0, 24, 3), (0, 32, 3), (0, 38, 3), (0, 53, 3), (1, 43, 3), (1, 50, 3), (1, 51, 3), (0, 45, 3),
    ),
    (
        (0, 21, 3), (0, 29, 3), (0, 52, 3), (0, 61, 3), (1, 41, 3), (1, 58, 3), (1, 59, 3), (1, 62, 3), (0, 55, 3),
        (1, 60, 3),
    ),
    (
        (0, 25, 3), (0, 44, 3), (0, 46, 3), (0, 47, 3), (1, 54, 3),
    ),
    (
        (0, 26, 3), (0, 33, 3), (0, 20, 3), (0, 39, 3), (0, 56, 3), (0, 7, 3), (0, 48, 3), (0, 37, 3),
    ),
    (
        (0, 50, 3), (0, 43, 3),
    ),
    (
        (0, 51, 3), (0, 41, 3), (0, 58, 3), (0, 62, 3), (0, 59, 3),
    ),
    (
        (0, 54, 3), (0, 60, 3),
    ),
    (),
    (),
    (),
    (),
    (),
)
PLANES = (0, 1, -1, 2)

GROUPS = 4
GTOK = 16
FILL = -1e30


def dispatch(index, branches, low=0, high=None):
    high = len(branches) if high is None else high
    if not any(branches[low:high]):
        return
    if high - low == 1:
        branches[low]()
        return
    mid = (low + high) // 2

    @pl.when(index < mid)
    def _():
        dispatch(index, branches, low, mid)

    @pl.when(index >= mid)
    def _():
        dispatch(index, branches, mid, high)


def kernel(
    stream_hbm, deltas_hbm, gain_hbm, unembed_hbm, targets_hbm, lse_ref, entropy_ref, logprob_ref,
    stream_v, deltas_v, targets_v, gain_v, gains, outbox, gat, words, rows_a, rows_b, acc, final,
    squares, scales, tops, sums, stats, from_x, stats_x, from_y, stats_y, from_z,
    load_sem, own_sem, words_send, words_recv, gain_send, gain_recv,
    part_send, part_recv, send_sem, recv_sem,
    x_send, x_recv, y_send, y_recv, z_send, z_recv,
):
    section = lax.axis_index("section")
    x = lax.axis_index("vocab_0")
    z = lax.axis_index("vocab_1")
    y = section // 2
    core = section % 2
    sign = 1 - 2 * core
    nwords = unembed_hbm.shape[0]
    plane_width = unembed_hbm.shape[1] // 4
    home = (x, y, z)

    def device(xx, yy, zz, cc):
        return (yy * 2 + cc, xx, zz)

    def moved(axis, step):
        at = list(home)
        at[axis] = lax.rem(at[axis] + step + 4, 4)
        return tuple(at)

    neighbours = [device(*moved(axis, way * sign), core) for axis, way in LINKS]
    partner = device(x, y, z, 1 - core)
    source = [{d: lax.rem(home[axis] - sign * d + 4, 4) for d in (-1, 0, 1, 2)} for axis in range(3)]

    loads = [
        pltpu.make_async_copy(stream_hbm, stream_v, load_sem.at[0]),
        pltpu.make_async_copy(deltas_hbm, deltas_v, load_sem.at[1]),
        pltpu.make_async_copy(targets_hbm, targets_v, load_sem.at[2]),
        pltpu.make_async_copy(gain_hbm, gain_v, load_sem.at[3]),
    ]
    for copy in loads:
        copy.start()

    barrier = pltpu.get_barrier_semaphore()
    for axis in range(3):
        for step in (1, 2, 3):
            at = moved(axis, step)
            pl.semaphore_signal(barrier, inc=1, device_id=device(*at, core), device_id_type=MESH)
            if axis == 2:
                pl.semaphore_signal(barrier, inc=1, device_id=device(*at, 1 - core), device_id_type=MESH)
    pl.semaphore_signal(barrier, inc=1, device_id=partner, device_id_type=MESH)

    def columns(plane):
        return pl.ds(pl.multiple_of(plane * plane_width, 128), plane_width)

    own_words = []
    for p, dx in enumerate(PLANES):
        plane = source[0][dx]
        own_words.append(
            pltpu.make_async_copy(
                unembed_hbm.at[:, columns(plane)], words.at[0, plane, pl.ds(0, nwords)], own_sem.at[p]
            )
        )
        own_words[-1].start()

    for copy in loads:
        copy.wait()

    lane = lax.broadcasted_iota(jnp.int32, (GTOK, 128), 1)
    low = lane < 64
    odd = lax.rem(z, 2) == 1
    my_slot = ((x * 4 + y) * 4 + z) * GROUPS

    first = jnp.where(section == 0, 1.0, 0.0).astype(F32)
    former = deltas_v[0].astype(F32) + stream_v[...].astype(F32) * first
    kept = former.astype(BF16).astype(F32)
    latter = deltas_v[1].astype(F32) + (former - kept)
    packed = []
    heads = []
    for value in (kept, latter):
        packed.append(jnp.where(odd, value[64:192], value[0:128]))
        packed.append(jnp.where(odd, value[192:320], value[128:256]))
        heads.append(jnp.where(odd, value[0:64], value[256:320]))
    lead = jnp.where(odd, heads[1], heads[0])
    trail = jnp.where(odd, heads[0], heads[1])
    packed.append(jnp.concatenate([lead, trail], axis=0))
    for k, value in enumerate(packed):
        tile = jnp.transpose(value).astype(BF16)
        for half in range(2):

            @pl.when(core == half)
            def _():
                for g in range(GROUPS):
                    t0 = half * 64 + g * GTOK
                    gat[my_slot + g, core, k] = tile[t0 : t0 + GTOK]

            @pl.when(core != half)
            def _():
                for g in range(GROUPS):
                    t0 = half * 64 + g * GTOK
                    outbox[g, k] = tile[t0 : t0 + GTOK]

    low_row = lax.broadcasted_iota(jnp.int32, (1, 128), 1) < 64
    none = jnp.zeros((1, 64), F32)
    g0 = gain_v[0:128].reshape(1, 128)
    g1 = gain_v[128:256].reshape(1, 128)
    g2 = jnp.concatenate([gain_v[256:320].reshape(1, 64), none], axis=1)
    t0, t1, t2 = (pltpu.roll(v, 64, 1) for v in (g0, g1, g2))
    blank = jnp.zeros((1, 128), F32)
    gain_rows = (
        (g0, blank),
        (g1, blank),
        (g2, jnp.where(low_row, 0.0, t0)),
        (blank, jnp.where(low_row, t0, t1)),
        (blank, jnp.where(low_row, t1, t2)),
    )
    gains[x * 4 + z] = jnp.concatenate(
        [jnp.where(odd, other, even) for even, other in gain_rows] + [blank] * 3, axis=0
    )

    final[:, 1184:1200, :] = jnp.full((2, 16, 256), FILL, F32)

    pl.semaphore_wait(barrier, 13)

    part = pltpu.make_async_remote_copy(
        src_ref=outbox,
        dst_ref=gat.at[pl.ds(my_slot, GROUPS), core],
        send_sem=part_send,
        recv_sem=part_recv,
        device_id=partner,
        device_id_type=MESH,
    )
    part.start()

    def gain_copy(n, link):
        at = (source[0][n[0]] * 4 + source[2][n[2]])
        place = (TREE_INDEX[child(n, link)] if link is not None else TREE_INDEX[n])
        return pltpu.make_async_remote_copy(
            src_ref=gains.at[at],
            dst_ref=gains.at[at],
            send_sem=gain_send.at[GAIN_INDEX[place]],
            recv_sem=gain_recv.at[GAIN_INDEX[place]],
            device_id=neighbours[link or 0],
            device_id_type=MESH,
        )

    def block_copy(n, row, link, g):
        slot = source[0][n[0]] * 64 + source[1][n[1]] * 16 + source[2][n[2]] * 4 + g
        return pltpu.make_async_remote_copy(
            src_ref=gat.at[slot],
            dst_ref=gat.at[slot],
            send_sem=send_sem.at[g],
            recv_sem=recv_sem.at[row * GROUPS + g],
            device_id=neighbours[link],
            device_id_type=MESH,
        )

    def send_gain(n):
        for row, (dx, dy, dz, link) in enumerate(TREE):
            if dy == 0 and parent((dx, dy, dz), link) == n:
                gain_copy(n, link).start()

    def run(actions):
        for kind, row, g in actions:
            dx, dy, dz, link = TREE[row]
            n = (dx, dy, dz)
            if kind == 0:
                block_copy(n, row, link, g).wait_recv()
                if g == 0 and dy == 0:
                    gain_copy(n, None).wait_recv()
                    send_gain(n)
            else:
                block_copy(parent(n, link), row, link, g).start()

    send_gain((0, 0, 0))

    their_words = []
    for p, dx in enumerate(PLANES):
        plane = lax.rem(x + sign * dx + 4, 4)
        their_words.append(
            pltpu.make_async_remote_copy(
                src_ref=unembed_hbm.at[:, columns(plane)],
                dst_ref=words.at[1, plane, pl.ds(0, nwords)],
                send_sem=words_send.at[p],
                recv_sem=words_recv.at[p],
                device_id=partner,
                device_id_type=MESH,
            )
        )

    for copy in their_words:
        copy.start()
    part.wait_recv()

    segment = lax.broadcasted_iota(jnp.int32, (1, 128), 1) // GTOK

    def spread(value):
        for step in (16, 32, 64):
            value = value + pltpu.roll(value, step, 1)
        return value

    def prepare(g, p, zp, rows):
        plane = source[0][PLANES[p]]
        running = [jnp.zeros((GTOK, 128), F32) for _ in range(5)]
        both = gains[plane * 4 + 2 * zp] + gains[plane * 4 + 2 * zp + 1]
        factor = [jnp.broadcast_to(both[k : k + 1, :], (GTOK, 128)) for k in range(5)]
        for yy in range(4):
            even = plane * 64 + yy * 16 + 2 * zp * 4 + g
            other = even + 4
            for cc in range(2):
                pe = gat[even, cc, 4].astype(F32)
                po = gat[other, cc, 4].astype(F32)
                for l in range(2):
                    layer = 4 * yy + 2 * cc + l
                    if l == 0:
                        middle = jnp.where(low, pe, po)
                    else:
                        middle = pltpu.roll(jnp.where(low, po, pe), 64, 1)
                    values = [
                        gat[even, cc, 2 * l].astype(F32),
                        gat[even, cc, 2 * l + 1].astype(F32),
                        middle,
                        gat[other, cc, 2 * l].astype(F32),
                        gat[other, cc, 2 * l + 1].astype(F32),
                    ]
                    span = slice(layer * GTOK, (layer + 1) * GTOK)
                    total = jnp.zeros((GTOK, 128), F32) if p == 0 and zp == 0 else squares[span, :]
                    for k in range(5):
                        at = 5 * zp + k
                        running[k] = running[k] + values[k]
                        total = total + running[k] * running[k]
                        rows[span, at * 128 : (at + 1) * 128] = (running[k] * factor[k]).astype(BF16)
                    squares[span, :] = total

    def multiply(p, stretch, rows):
        start, stop = ((0, 592), (592, nwords))[stretch]
        plane = source[0][PLANES[p]]
        most = []
        for half in range(2):
            product = lax.dot_general(
                words[half, plane, start:stop, :], rows[...], (((1,), (1,)), ((), ())), preferred_element_type=F32
            )
            if p == 0:
                acc[half, start:stop, :] = product
            elif p < 3:
                acc[half, start:stop, :] = acc[half, start:stop, :] + product
            else:
                total = acc[half, start:stop, :] + product
                final[half, start:stop, :] = total
                most.append(jnp.max(total[0:592].reshape(74, 8, 256), axis=0))
                if stop - start > 592:
                    most.append(jnp.broadcast_to(jnp.max(total[592:], axis=0, keepdims=True), (8, 256)))
        if p == 3:
            if stretch == 1:
                most.append(tops[...])
            tops[...] = functools.reduce(jnp.maximum, most)

    def scaled():
        total = jnp.sum(jnp.transpose(squares[...]), axis=0, keepdims=True)
        scales[0:1, :] = lax.rsqrt(total / (4 * plane_width) + EPSILON)

    def peaked():
        scales[1:2, :] = jnp.max(tops[...], axis=0, keepdims=True) * scales[0:1, :]

    def folded(g, half):
        scale = jnp.broadcast_to(scales[0:1, :], (8, 256))
        peaks = jnp.broadcast_to(scales[1:2, :], (8, 256))
        sublane = lax.broadcasted_iota(jnp.int32, (8, 256), 0)
        holder = core if half == 0 else 1 - core
        first_word = (((y * 2 + holder) * 4 + x) * 4 + z) * nwords
        local = targets_v[...].reshape(1, 128) - first_word
        local = jnp.where(local < nwords, local, -8)
        local = spread(jnp.where(segment == core * GROUPS + g, local, 0))
        wanted = jnp.broadcast_to(jnp.concatenate([local, local], axis=1), (8, 256)) - sublane
        if half == 0:
            mass = moment = picked = jnp.zeros((8, 256), F32)
        else:
            mass, moment, picked = (sums[k] for k in range(3))
        for k in range(150):
            z_all = final[half, 8 * k : 8 * k + 8, :] * scale
            z_rel = z_all - peaks
            e = jnp.exp(z_rel)
            mass = mass + e
            moment = moment + e * z_rel
            picked = jnp.where(wanted == 8 * k, z_all, picked)
        if half == 0:
            for k, value in enumerate((mass, moment, picked)):
                sums[k] = value
            return
        found = [scales[1:2, :]] + [jnp.sum(v, axis=0, keepdims=True) for v in (mass, moment, picked)]
        for k, value in enumerate(found):
            stats[g, 2 * k : 2 * k + 1, :] = value[:, 0:128]
            stats[g, 2 * k + 1 : 2 * k + 2, :] = value[:, 128:256]

    def place(p, k, g):
        dispatch(g, [functools.partial(run, PLAN[1 + 2 * (4 * j + p) + k]) if PLAN[1 + 2 * (4 * j + p) + k] else None for j in range(GROUPS)])

    run(PLAN[0])
    for zp in range(2):
        prepare(0, 0, zp, rows_a)

    def body(g, carry):
        for p in range(4):
            now, later = (rows_a, rows_b) if p % 2 == 0 else (rows_b, rows_a)
            following = (g, p + 1) if p < 3 else (jnp.minimum(g + 1, GROUPS - 1), 0)
            former_group = lax.rem(g + GROUPS - 1, GROUPS)
            place(p, 0, g)

            @pl.when(g == 0)
            def _():
                plane = source[0][PLANES[p]]
                own_words[p].wait()
                pltpu.make_async_remote_copy(
                    src_ref=unembed_hbm.at[:, columns(plane)],
                    dst_ref=words.at[1, plane, pl.ds(0, nwords)],
                    send_sem=words_send.at[p],
                    recv_sem=words_recv.at[p],
                    device_id=partner,
                    device_id_type=MESH,
                ).wait_recv()

            if p == 3:
                scaled()
            for k in range(2):
                if k == 1:
                    place(p, 1, g)
                multiply(p, k, now)
                prepare(*following, k, later)
                if p == 0:
                    folded(former_group, k)
            if p == 3:
                peaked()
        return carry

    lax.fori_loop(0, GROUPS, body, 0)
    run(PLAN[33])
    for half in range(2):
        folded(GROUPS - 1, half)

    def joined(parts):
        tops = [part[:, 0:2, :] for part in parts]
        most = functools.reduce(jnp.maximum, tops)
        shifts = [top - most for top in tops]
        factors = [jnp.exp(shift) for shift in shifts]
        mass = sum(f * part[:, 2:4, :] for f, part in zip(factors, parts))
        moment = sum(
            f * (part[:, 4:6, :] + shift * part[:, 2:4, :]) for f, shift, part in zip(factors, shifts, parts)
        )
        picked = sum(part[:, 6:8, :] for part in parts)
        return most, mass, moment, picked

    waits = []

    def exchanged(axis, mine, inbox, send, recv, result):
        copies = []
        for step in (1, 2, 3):
            copies.append(
                pltpu.make_async_remote_copy(
                    src_ref=mine,
                    dst_ref=inbox.at[step - 1],
                    send_sem=send.at[step - 1],
                    recv_sem=recv.at[step - 1],
                    device_id=device(*moved(axis, step), core),
                    device_id_type=MESH,
                )
            )
        for copy in copies:
            copy.start()
        for copy in copies:
            copy.wait_recv()
        waits.extend(copies)
        for k, value in enumerate(joined([mine[...]] + [inbox[k] for k in range(3)])):
            result[:, 2 * k : 2 * k + 2, :] = value

    exchanged(0, stats, from_x, x_send, x_recv, stats_x)
    exchanged(1, stats_x, from_y, y_send, y_recv, stats_y)

    def last_copy(step, other, towards):
        cc = 1 - core if other else core
        origin = core if towards else cc
        return pltpu.make_async_remote_copy(
            src_ref=stats_y,
            dst_ref=from_z.at[origin, step],
            send_sem=z_send.at[4 * other + step],
            recv_sem=z_recv.at[4 * other + step],
            device_id=device(*moved(2, step), cc),
            device_id_type=MESH,
        )

    lasts = [(1, True), (2, True), (3, True), (1, False), (2, False), (3, False), (0, True)]
    for step, other in lasts:
        last_copy(step, other, True).start()
    from_z[core, 0] = stats_y[...]
    for step, other in lasts:
        last_copy(step, other, False).wait_recv()
    found = [[], [], []]
    for half in range(2):
        most, mass, moment, picked = joined([from_z[half, k] for k in range(4)])
        log_mass = jnp.log(mass)
        lse = most + log_mass
        for k, value in enumerate((lse, log_mass - moment / mass, picked - lse)):
            found[k].append(jnp.where(y < 2, value[:, 0, :], value[:, 1, :]))
    grid_segment = lax.broadcasted_iota(jnp.int32, (8, 128), 1) // GTOK
    grid_row = lax.broadcasted_iota(jnp.int32, (8, 128), 0)
    for parts, out_ref in zip(found, (lse_ref, entropy_ref, logprob_ref)):
        grid = jnp.concatenate(parts, axis=0)
        for l in range(2):
            layer = lax.rem(4 * y + 2 * core, 8) + l
            value = spread(jnp.where(grid_segment == layer, grid, 0.0))
            out_ref[l : l + 1, :] = jnp.sum(jnp.where(grid_segment == grid_row, value, 0.0), axis=0, keepdims=True)

    for step, other in lasts:
        last_copy(step, other, True).wait_send()
    for copy in waits:
        copy.wait_send()
    part.wait_send()
    for copy in their_words:
        copy.wait_send()
    for row, (dx, dy, dz, link) in enumerate(TREE):
        if dy == 0:
            gain_copy(parent((dx, dy, dz), link), link).wait_send()
    for g in range(GROUPS):
        pltpu.make_async_remote_copy(
            src_ref=gat.at[pl.ds(0, len(TREE))],
            dst_ref=gat.at[pl.ds(0, len(TREE))],
            send_sem=send_sem.at[g],
            recv_sem=recv_sem.at[0],
            device_id=neighbours[0],
            device_id_type=MESH,
        ).wait_send()


def wrapped(c):
    return (c + 1) % 4 - 1


def parent(n, link):
    axis, way = LINKS[link]
    n = list(n)
    n[axis] = wrapped(n[axis] - way)
    return tuple(n)


def child(n, link):
    axis, way = LINKS[link]
    n = list(n)
    n[axis] = wrapped(n[axis] + way)
    return tuple(n)


TREE_INDEX = {row[:3]: k for k, row in enumerate(TREE)}
GAIN_INDEX = {k: i for i, k in enumerate(k for k, row in enumerate(TREE) if row[1] == 0)}


def shards(stream_in, deltas, norm_gain, unembed, targets):
    nwords, width = unembed.shape
    anywhere = pl.BlockSpec(memory_space=pl.ANY)
    inside = pl.BlockSpec(memory_space=pltpu.VMEM)
    dma = pltpu.SemaphoreType.DMA
    return pl.pallas_call(
        kernel,
        out_shape=(jax.ShapeDtypeStruct((2, 128), F32),) * 3,
        in_specs=[anywhere] * 5,
        out_specs=(inside,) * 3,
        scratch_shapes=[
            pltpu.VMEM((320, 128), BF16),
            pltpu.VMEM((2, 320, 128), BF16),
            pltpu.VMEM((128,), jnp.int32),
            pltpu.VMEM((320,), F32),
            pltpu.VMEM((16, 8, 128), F32),
            pltpu.VMEM((GROUPS, 5, GTOK, 128), BF16),
            pltpu.VMEM((64 * GROUPS, 2, 5, GTOK, 128), BF16),
            pltpu.VMEM((2, 4, nwords, width // 4), BF16),
            pltpu.VMEM((256, width // 4), BF16),
            pltpu.VMEM((256, width // 4), BF16),
            pltpu.VMEM((2, 1200, 256), F32),
            pltpu.VMEM((2, 1200, 256), F32),
            pltpu.VMEM((256, 128), F32),
            pltpu.VMEM((8, 256), F32),
            pltpu.VMEM((8, 256), F32),
            pltpu.VMEM((3, 8, 256), F32),
            pltpu.VMEM((GROUPS, 8, 128), F32),
            pltpu.VMEM((3, GROUPS, 8, 128), F32),
            pltpu.VMEM((GROUPS, 8, 128), F32),
            pltpu.VMEM((3, GROUPS, 8, 128), F32),
            pltpu.VMEM((GROUPS, 8, 128), F32),
            pltpu.VMEM((2, 4, GROUPS, 8, 128), F32),
            dma((4,)),
            dma((4,)),
            dma((4,)),
            dma((4,)),
            dma((15,)),
            dma((15,)),
            dma,
            dma,
            dma((GROUPS,)),
            dma((63 * GROUPS,)),
            dma((3,)),
            dma((3,)),
            dma((3,)),
            dma((3,)),
            dma((8,)),
            dma((8,)),
        ],
        compiler_params=pltpu.CompilerParams(
            collective_id=0, has_side_effects=True, vmem_limit_bytes=60 * 1024 * 1024
        ),
    )(stream_in.T, deltas.transpose(0, 2, 1), norm_gain, unembed, targets)


def solution(mesh):
    torus = Mesh(
        mesh.devices.reshape(mesh.shape["section"], 4, 4), ("section", "vocab_0", "vocab_1")
    )
    placed = (P(None, VOCAB), P("section", None, VOCAB), P(VOCAB), P(SECTION_VOCAB, None), P())
    return jax.shard_map(
        shards,
        mesh=torus,
        in_specs=placed,
        out_specs=(P("section", None), P("section", None), P("section", None)),
        check_vma=False,
    )
```

```python
import functools

import jax
import jax.numpy as jnp
from jax import lax
from jax.experimental import pallas as pl
from jax.experimental.pallas import tpu as pltpu
from jax.sharding import Mesh
from jax.sharding import PartitionSpec as P

MESH = pl.DeviceIdType.MESH
F32 = jnp.float32
BF16 = jnp.bfloat16
EPSILON = 1e-06

VOCAB = ("vocab_0", "vocab_1")
SECTION_VOCAB = ("section", "vocab_0", "vocab_1")

LINKS = ((0, 1), (0, -1), (1, 1), (1, -1), (2, 1), (2, -1))
TREE = (
    (-1, 0, 0, 1), (0, -1, 0, 3), (0, 0, -1, 5), (0, 0, 1, 4), (0, 1, 0, 2), (1, 0, 0, 0),
    (-1, -1, 0, 1), (-1, 0, -1, 1), (-1, 0, 1, 1), (-1, 1, 0, 1), (0, -1, -1, 5), (0, -1, 1, 4),
    (0, 0, 2, 4), (0, 1, -1, 5), (0, 1, 1, 2), (0, 2, 0, 2), (1, -1, 0, 3), (1, 0, -1, 0),
    (1, 0, 1, 0), (1, 1, 0, 2), (2, 0, 0, 0), (-1, -1, -1, 3), (-1, -1, 1, 1), (-1, 0, 2, 5),
    (-1, 1, -1, 5), (-1, 1, 1, 1), (-1, 2, 0, 2), (0, -1, 2, 4), (0, 1, 2, 2), (0, 2, -1, 3),
    (0, 2, 1, 3), (1, -1, -1, 0), (1, -1, 1, 4), (1, 0, 2, 4), (1, 1, -1, 2), (1, 1, 1, 2),
    (1, 2, 0, 3), (2, -1, 0, 0), (2, 0, -1, 0), (2, 0, 1, 0), (2, 1, 0, 0), (-1, -1, 2, 4),
    (-1, 1, 2, 5), (-1, 2, -1, 5), (-1, 2, 1, 3), (0, 2, 2, 5), (1, -1, 2, 5), (1, 1, 2, 4),
    (1, 2, -1, 0), (1, 2, 1, 3), (2, -1, -1, 0), (2, -1, 1, 3), (2, 0, 2, 5), (2, 1, -1, 1),
    (2, 1, 1, 1), (2, 2, 0, 3), (-1, 2, 2, 4), (1, 2, 2, 4), (2, -1, 2, 3), (2, 1, 2, 5),
    (2, 2, -1, 2), (2, 2, 1, 1), (2, 2, 2, 1),
)
PLAN = (
    (
        (1, 0, 0), (1, 1, 0), (1, 2, 0), (1, 3, 0), (1, 4, 0), (1, 5, 0), (1, 0, 1), (1, 1, 1), (1, 2, 1),
        (1, 3, 1), (1, 4, 1), (1, 5, 1), (1, 0, 2), (1, 1, 2), (1, 2, 2), (1, 3, 2), (1, 4, 2), (1, 5, 2),
        (1, 0, 3), (1, 1, 3), (1, 2, 3), (1, 3, 3), (1, 4, 3), (1, 5, 3), (0, 0, 0), (0, 1, 0), (0, 2, 0),
        (0, 3, 0), (0, 4, 0), (0, 5, 0), (1, 9, 0), (1, 10, 0), (1, 11, 0), (1, 14, 0), (1, 16, 0), (1, 17, 0),
        (1, 18, 0), (0, 0, 1), (0, 1, 1), (0, 2, 1), (0, 3, 1), (0, 4, 1), (0, 5, 1), (1, 9, 1), (1, 10, 1),
        (1, 11, 1), (1, 14, 1), (1, 16, 1), (1, 7, 0), (1, 17, 1), (0, 0, 2), (0, 1, 2), (0, 2, 2), (0, 3, 2),
        (0, 4, 2), (0, 5, 2), (1, 10, 2), (1, 11, 2), (1, 14, 2), (1, 16, 2), (1, 9, 2), (1, 18, 1), (0, 0, 3),
        (0, 1, 3), (0, 2, 3), (0, 3, 3), (0, 4, 3), (0, 5, 3), (1, 10, 3), (1, 11, 3), (1, 14, 3), (1, 16, 3),
        (1, 6, 0), (1, 12, 0), (1, 13, 0), (1, 15, 0), (1, 17, 2), (1, 12, 1), (1, 15, 1), (0, 9, 0), (0, 10, 0),
        (0, 11, 0), (0, 14, 0), (0, 16, 0), (0, 17, 0), (1, 22, 0), (1, 24, 0), (1, 29, 0), (1, 38, 0), (1, 13, 1),
        (1, 31, 0), (1, 32, 0), (0, 9, 1), (0, 10, 1), (0, 11, 1), (0, 14, 1), (0, 16, 1), (0, 18, 0), (1, 22, 1),
        (1, 29, 1), (1, 35, 0), (1, 25, 0), (1, 12, 2), (1, 13, 2), (1, 19, 0), (1, 39, 0), (0, 7, 0), (0, 10, 2),
        (0, 11, 2), (0, 14, 2), (0, 16, 2), (0, 17, 1), (1, 29, 2), (1, 22, 2), (1, 12, 3), (1, 13, 3), (1, 15, 2),
        (1, 37, 0), (0, 9, 2), (0, 10, 3), (0, 11, 3), (0, 14, 3), (0, 16, 3), (0, 18, 1), (1, 29, 3), (1, 30, 0),
        (1, 8, 0), (1, 27, 0), (0, 6, 0), (0, 12, 0), (0, 13, 0), (0, 15, 0), (0, 17, 2), (1, 28, 0), (0, 29, 0),
        (1, 45, 0), (1, 48, 0), (1, 27, 1), (1, 38, 1), (0, 22, 0), (0, 24, 0), (0, 12, 1), (0, 15, 1), (0, 38, 0),
        (1, 44, 0), (1, 28, 1), (1, 53, 0), (1, 30, 1), (0, 29, 1), (1, 45, 1), (1, 7, 1), (1, 27, 2), (1, 15, 3),
        (1, 31, 1), (0, 22, 1), (0, 13, 1), (0, 31, 0), (0, 32, 0), (0, 35, 0), (1, 49, 0), (0, 29, 2), (1, 45, 2),
        (1, 25, 1), (1, 27, 3), (1, 18, 2), (0, 25, 0), (0, 12, 2), (0, 13, 2), (0, 19, 0), (0, 39, 0), (1, 28, 2),
        (1, 30, 2), (0, 29, 3), (1, 45, 3), (1, 24, 1), (1, 32, 1), (1, 50, 0), (1, 54, 0), (0, 22, 2), (0, 12, 3),
        (0, 13, 3), (0, 15, 2), (0, 37, 0), (1, 28, 3), (1, 30, 3), (0, 30, 0), (1, 26, 0), (1, 20, 0), (1, 52, 0),
        (0, 8, 0), (0, 27, 0), (0, 28, 0), (0, 45, 0), (0, 48, 0),
    ),
    (
        (1, 44, 1), (0, 44, 0), (1, 56, 0), (1, 61, 0),
    ),
    (
        (1, 9, 3), (1, 46, 0), (1, 34, 0), (1, 47, 0), (1, 40, 0), (0, 27, 1), (0, 28, 1), (0, 45, 1), (0, 38, 1),
        (0, 53, 0), (1, 36, 0), (0, 30, 1),
    ),
    (
        (1, 22, 3), (1, 23, 0), (1, 17, 3), (1, 35, 1), (0, 7, 1), (0, 27, 2), (0, 15, 3), (0, 45, 2), (0, 31, 1),
        (1, 21, 0), (0, 49, 0), (1, 57, 0),
    ),
    (
        (1, 6, 1), (1, 42, 0), (1, 33, 0), (1, 19, 1), (1, 39, 1), (0, 25, 1), (0, 27, 3), (0, 28, 2), (0, 45, 3),
        (0, 18, 2), (0, 30, 2),
    ),
    (
        (1, 41, 0), (1, 26, 1), (1, 37, 1), (1, 59, 0), (0, 24, 1), (0, 28, 3), (0, 32, 1), (0, 50, 0), (0, 54, 0),
        (1, 49, 1), (1, 53, 1), (1, 51, 0), (0, 30, 3),
    ),
    (
        (1, 48, 1), (1, 60, 0), (0, 26, 0), (0, 56, 0), (0, 20, 0), (0, 52, 0), (0, 61, 0), (1, 43, 0), (1, 62, 0),
        (1, 58, 0), (0, 44, 1), (1, 56, 1),
    ),
    (
        (1, 8, 1), (1, 24, 2), (1, 32, 2), (1, 34, 1), (1, 38, 2), (0, 9, 3), (0, 46, 0), (0, 34, 0), (0, 47, 0),
        (0, 40, 0), (1, 55, 0), (0, 36, 0),
    ),
    (
        (1, 7, 2), (1, 31, 2), (1, 35, 2), (1, 52, 1), (0, 22, 3), (0, 23, 0), (0, 17, 3), (0, 35, 1), (0, 57, 0),
        (1, 47, 1), (1, 44, 2), (0, 21, 0), (1, 25, 2), (1, 46, 1), (1, 18, 3), (1, 19, 2), (0, 6, 1), (0, 42, 0),
        (0, 33, 0), (0, 19, 1), (0, 39, 1),
    ),
    (
        (1, 36, 1), (0, 49, 1), (1, 57, 1), (1, 23, 1), (1, 26, 2), (1, 33, 1), (1, 50, 1), (1, 54, 1), (0, 41, 0),
        (0, 26, 1), (0, 37, 1), (0, 53, 1), (0, 59, 0),
    ),
    (
        (1, 21, 1), (0, 51, 0), (1, 41, 1), (1, 42, 1), (1, 20, 1), (1, 60, 1), (0, 43, 0), (0, 56, 1), (0, 48, 1),
        (0, 60, 0), (0, 62, 0), (1, 62, 1),
    ),
    (
        (0, 58, 0), (1, 43, 1), (1, 32, 3), (1, 34, 2), (1, 40, 1), (1, 61, 1), (0, 8, 1), (0, 24, 2), (0, 32, 2),
        (0, 34, 1), (0, 38, 2), (1, 49, 2),
    ),
    (
        (1, 51, 1), (0, 55, 0), (1, 19, 3), (1, 39, 2), (1, 53, 2), (1, 59, 1), (0, 7, 2), (0, 31, 2), (0, 35, 2),
        (0, 47, 1), (0, 52, 1), (1, 58, 1),
    ),
    (
        (0, 44, 2), (1, 56, 2), (1, 6, 2), (1, 24, 3), (1, 47, 2), (1, 37, 2), (0, 25, 2), (0, 46, 1), (0, 18, 3),
        (0, 19, 2), (0, 57, 1), (1, 35, 3), (1, 55, 1),
    ),
    (
        (0, 36, 1), (1, 8, 2), (1, 26, 3), (1, 33, 2), (1, 48, 2), (1, 52, 2), (0, 23, 1), (0, 26, 2), (0, 33, 1),
        (0, 50, 1), (0, 54, 1), (1, 44, 3),
    ),
    (
        (0, 21, 1), (1, 7, 3), (1, 46, 2), (1, 34, 3), (1, 38, 3), (0, 41, 1), (0, 42, 1), (0, 20, 1), (0, 60, 1),
        (0, 62, 1), (1, 36, 2), (0, 49, 2), (1, 57, 2),
    ),
    (
        (1, 41, 2), (1, 23, 2), (1, 25, 3), (1, 31, 3), (0, 43, 1), (0, 32, 3), (0, 34, 2), (0, 40, 1), (0, 61, 1),
        (1, 49, 3), (0, 51, 1),
    ),
    (
        (1, 42, 2), (1, 33, 3), (1, 50, 2), (0, 56, 2), (0, 19, 3), (0, 39, 2), (0, 53, 2), (0, 59, 1), (1, 60, 2),
        (1, 62, 2), (1, 21, 2), (0, 58, 1),
    ),
    (
        (1, 43, 2), (1, 20, 2), (1, 54, 2), (0, 6, 2), (0, 24, 3), (0, 35, 3), (0, 47, 2), (0, 37, 2), (1, 47, 3),
        (1, 51, 2), (0, 55, 1), (1, 40, 2), (1, 59, 2), (1, 61, 2),
    ),
    (
        (0, 8, 2), (0, 26, 3), (0, 33, 2), (0, 48, 2), (0, 52, 2), (1, 58, 2), (0, 44, 3), (1, 56, 3), (1, 41, 3),
        (1, 39, 3), (1, 53, 3),
    ),
    (
        (0, 7, 3), (0, 46, 2), (0, 34, 3), (0, 57, 2), (0, 38, 3), (1, 52, 3), (1, 55, 2), (0, 36, 2), (1, 6, 3),
        (1, 37, 3),
    ),
    (
        (0, 41, 2), (0, 23, 2), (0, 25, 3), (0, 31, 3), (1, 46, 3), (1, 36, 3), (0, 49, 3), (0, 60, 2), (1, 57, 3),
        (1, 8, 3), (1, 23, 3), (1, 48, 3), (0, 42, 2), (0, 33, 3), (0, 50, 2), (0, 62, 2),
    ),
    (
        (1, 21, 3), (0, 21, 2), (1, 42, 3), (1, 50, 3), (1, 54, 3), (0, 43, 2), (0, 47, 3), (0, 20, 2), (0, 54, 2),
    ),
    (
        (0, 51, 2), (1, 43, 3), (1, 20, 3), (0, 56, 3), (0, 40, 2), (0, 59, 2), (0, 61, 2), (1, 62, 3),
    ),
    (
        (0, 58, 2), (1, 40, 3), (1, 61, 3), (0, 41, 3), (0, 39, 3), (0, 52, 3), (0, 53, 3), (1, 51, 3), (1, 59, 3),
        (1, 60, 3), (1, 58, 3), (0, 55, 2),
    ),
    (
        (0, 6, 3), (0, 46, 3), (0, 57, 3), (0, 37, 3), (1, 55, 3), (0, 36, 3),
    ),
    (
        (0, 8, 3), (0, 23, 3), (0, 48, 3), (0, 21, 3),
    ),
    (
        (0, 42, 3), (0, 50, 3), (0, 54, 3),
    ),
    (
        (0, 43, 3), (0, 20, 3), (0, 62, 3), (0, 51, 3), (0, 60, 3),
    ),
    (
        (0, 40, 3), (0, 59, 3), (0, 61, 3), (0, 58, 3),
    ),
    (
        (0, 55, 3),
    ),
    (),
    (),
    (),
    (),
)
PLANES = (0, 1, -1, 2)

GROUPS = 4
GTOK = 16
FILL = -1e30


def dispatch(index, branches, low=0, high=None):
    high = len(branches) if high is None else high
    if not any(branches[low:high]):
        return
    if high - low == 1:
        branches[low]()
        return
    mid = (low + high) // 2

    @pl.when(index < mid)
    def _():
        dispatch(index, branches, low, mid)

    @pl.when(index >= mid)
    def _():
        dispatch(index, branches, mid, high)


def kernel(
    stream_hbm, deltas_hbm, gain_hbm, unembed_hbm, targets_hbm, out_ref,
    stream_v, deltas_v, targets_v, gain_v, gains, outbox, gat, words, rows_a, rows_b, rows_c, acc, final,
    squares, scales, tops, sums, stats, slices, from_section, partial, from_plane,
    load_sem, own_sem, words_send, words_recv, gain_send, gain_recv,
    part_send, part_recv, send_sem, recv_sem,
    section_send, section_recv, plane_send, plane_recv,
):
    section = lax.axis_index("section")
    x = lax.axis_index("vocab_0")
    z = lax.axis_index("vocab_1")
    y = section // 2
    core = section % 2
    sign = 1 - 2 * core
    nwords = unembed_hbm.shape[0]
    plane_width = unembed_hbm.shape[1] // 4
    home = (x, y, z)

    def device(xx, yy, zz, cc):
        return (yy * 2 + cc, xx, zz)

    def moved(axis, step):
        at = list(home)
        at[axis] = lax.rem(at[axis] + step + 4, 4)
        return tuple(at)

    neighbours = [device(*moved(axis, way * sign), core) for axis, way in LINKS]
    partner = device(x, y, z, 1 - core)
    source = [{d: lax.rem(home[axis] - sign * d + 4, 4) for d in (-1, 0, 1, 2)} for axis in range(3)]

    loads = [
        pltpu.make_async_copy(stream_hbm, stream_v, load_sem.at[0]),
        pltpu.make_async_copy(deltas_hbm, deltas_v, load_sem.at[1]),
        pltpu.make_async_copy(targets_hbm, targets_v, load_sem.at[2]),
        pltpu.make_async_copy(gain_hbm, gain_v, load_sem.at[3]),
    ]
    for copy in loads:
        copy.start()

    def plane_peer(step):
        return device(lax.rem(x + step // 4, 4), y, lax.rem(z + step % 4, 4), core)

    def section_peer(step, other):
        return device(x, lax.rem(y + step, 4), z, 1 - core if other else core)

    section_peers = [(step, other) for step in range(4) for other in (0, 1) if step or other]
    barrier = pltpu.get_barrier_semaphore()
    around = [device(*moved(axis, way), cc) for axis, way in LINKS for cc in range(2)]
    for peer in around + [partner]:
        pl.semaphore_signal(barrier, inc=1, device_id=peer, device_id_type=MESH)

    def columns(plane):
        return pl.ds(pl.multiple_of(plane * plane_width, 128), plane_width)

    own_words = []
    for p, dx in enumerate(PLANES):
        plane = source[0][dx]
        own_words.append(
            pltpu.make_async_copy(
                unembed_hbm.at[:, columns(plane)], words.at[0, plane, pl.ds(0, nwords)], own_sem.at[p]
            )
        )
        own_words[-1].start()

    for copy in loads:
        copy.wait()

    lane = lax.broadcasted_iota(jnp.int32, (GTOK, 128), 1)
    low = lane < 64
    odd = lax.rem(z, 2) == 1
    my_slot = ((x * 4 + y) * 4 + z) * GROUPS

    first = jnp.where(section == 0, 1.0, 0.0).astype(F32)
    former = deltas_v[0].astype(F32) + stream_v[...].astype(F32) * first
    kept = former.astype(BF16).astype(F32)
    latter = deltas_v[1].astype(F32) + (former - kept)
    packed = []
    heads = []
    for value in (kept, latter):
        packed.append(jnp.where(odd, value[64:192], value[0:128]))
        packed.append(jnp.where(odd, value[192:320], value[128:256]))
        heads.append(jnp.where(odd, value[0:64], value[256:320]))
    lead = jnp.where(odd, heads[1], heads[0])
    trail = jnp.where(odd, heads[0], heads[1])
    packed.append(jnp.concatenate([lead, trail], axis=0))
    for k, value in enumerate(packed):
        tile = jnp.transpose(value).astype(BF16)
        for half in range(2):

            @pl.when(core == half)
            def _():
                for g in range(GROUPS):
                    t0 = half * 64 + g * GTOK
                    gat[my_slot + g, core, k] = tile[t0 : t0 + GTOK]

            @pl.when(core != half)
            def _():
                for g in range(GROUPS):
                    t0 = half * 64 + g * GTOK
                    outbox[g, k] = tile[t0 : t0 + GTOK]

    low_row = lax.broadcasted_iota(jnp.int32, (1, 128), 1) < 64
    none = jnp.zeros((1, 64), F32)
    g0 = gain_v[0:128].reshape(1, 128)
    g1 = gain_v[128:256].reshape(1, 128)
    g2 = jnp.concatenate([gain_v[256:320].reshape(1, 64), none], axis=1)
    t0, t1, t2 = (pltpu.roll(v, 64, 1) for v in (g0, g1, g2))
    blank = jnp.zeros((1, 128), F32)
    gain_rows = (
        (g0, blank),
        (g1, blank),
        (g2, jnp.where(low_row, 0.0, t0)),
        (blank, jnp.where(low_row, t0, t1)),
        (blank, jnp.where(low_row, t1, t2)),
    )
    gains[x * 4 + z] = jnp.concatenate(
        [jnp.where(odd, other, even) for even, other in gain_rows] + [blank] * 3, axis=0
    )

    final[:, 1184:1200, :] = jnp.full((2, 16, 256), FILL, F32)

    pl.semaphore_wait(barrier, 13)

    part = pltpu.make_async_remote_copy(
        src_ref=outbox,
        dst_ref=gat.at[pl.ds(my_slot, GROUPS), core],
        send_sem=part_send,
        recv_sem=part_recv,
        device_id=partner,
        device_id_type=MESH,
    )
    part.start()

    def gain_copy(n, link):
        at = (source[0][n[0]] * 4 + source[2][n[2]])
        place = (TREE_INDEX[child(n, link)] if link is not None else TREE_INDEX[n])
        return pltpu.make_async_remote_copy(
            src_ref=gains.at[at],
            dst_ref=gains.at[at],
            send_sem=gain_send.at[GAIN_INDEX[place]],
            recv_sem=gain_recv.at[GAIN_INDEX[place]],
            device_id=neighbours[link or 0],
            device_id_type=MESH,
        )

    def block_copy(n, row, link, g):
        slot = source[0][n[0]] * 64 + source[1][n[1]] * 16 + source[2][n[2]] * 4 + g
        return pltpu.make_async_remote_copy(
            src_ref=gat.at[slot],
            dst_ref=gat.at[slot],
            send_sem=send_sem.at[g],
            recv_sem=recv_sem.at[row * GROUPS + g],
            device_id=neighbours[link],
            device_id_type=MESH,
        )

    def first_copy(row, link, g, away):
        axis, way = LINKS[link]
        return pltpu.make_async_remote_copy(
            src_ref=outbox.at[g] if away else gat.at[my_slot + g, core],
            dst_ref=gat.at[my_slot + g, core],
            send_sem=send_sem.at[g],
            recv_sem=recv_sem.at[row * GROUPS + g],
            device_id=device(*moved(axis, -way * sign), 1 - core) if away else neighbours[link],
            device_id_type=MESH,
        )

    def send_gain(n):
        for row, (dx, dy, dz, link) in enumerate(TREE):
            if dy == 0 and parent((dx, dy, dz), link) == n:
                gain_copy(n, link).start()

    def run(actions):
        for kind, row, g in actions:
            dx, dy, dz, link = TREE[row]
            n = (dx, dy, dz)
            if kind == 0:
                block_copy(n, row, link, g).wait_recv()
                if g == 0 and dy == 0:
                    gain_copy(n, None).wait_recv()
                    send_gain(n)
            elif parent(n, link) == (0, 0, 0):
                for away in (False, True):
                    first_copy(row, link, g, away).start()
            else:
                block_copy(parent(n, link), row, link, g).start()

    send_gain((0, 0, 0))

    their_words = []
    for p, dx in enumerate(PLANES):
        plane = lax.rem(x + sign * dx + 4, 4)
        their_words.append(
            pltpu.make_async_remote_copy(
                src_ref=unembed_hbm.at[:, columns(plane)],
                dst_ref=words.at[1, plane, pl.ds(0, nwords)],
                send_sem=words_send.at[p],
                recv_sem=words_recv.at[p],
                device_id=partner,
                device_id_type=MESH,
            )
        )

    for copy in their_words:
        copy.start()

    segment = lax.broadcasted_iota(jnp.int32, (1, 128), 1) // GTOK

    def spread(value):
        for step in (16, 32, 64):
            value = value + pltpu.roll(value, step, 1)
        return value

    def prepare(g, p, zp, rows):
        plane = source[0][PLANES[p]]
        running = [jnp.zeros((GTOK, 128), F32) for _ in range(5)]
        both = gains[plane * 4 + 2 * zp] + gains[plane * 4 + 2 * zp + 1]
        factor = [jnp.broadcast_to(both[k : k + 1, :], (GTOK, 128)) for k in range(5)]
        for yy in range(4):
            even = plane * 64 + yy * 16 + 2 * zp * 4 + g
            other = even + 4
            for cc in range(2):
                pe = gat[even, cc, 4].astype(F32)
                po = gat[other, cc, 4].astype(F32)
                for l in range(2):
                    layer = 4 * yy + 2 * cc + l
                    if l == 0:
                        middle = jnp.where(low, pe, po)
                    else:
                        middle = pltpu.roll(jnp.where(low, po, pe), 64, 1)
                    values = [
                        gat[even, cc, 2 * l].astype(F32),
                        gat[even, cc, 2 * l + 1].astype(F32),
                        middle,
                        gat[other, cc, 2 * l].astype(F32),
                        gat[other, cc, 2 * l + 1].astype(F32),
                    ]
                    span = slice(layer * GTOK, (layer + 1) * GTOK)
                    total = jnp.zeros((GTOK, 128), F32) if p == 0 and zp == 0 else squares[g, span, :]
                    for k in range(5):
                        at = 5 * zp + k
                        running[k] = running[k] + values[k]
                        total = total + running[k] * running[k]
                        rows[span, at * 128 : (at + 1) * 128] = (running[k] * factor[k]).astype(BF16)
                    squares[g, span, :] = total

    def multiply(g, p, stretch, rows):
        start, stop = ((0, 592), (592, nwords))[stretch]
        plane = source[0][PLANES[p]]
        most = []
        for half in range(2):
            product = lax.dot_general(
                words[half, plane, start:stop, :], rows[...], (((1,), (1,)), ((), ())), preferred_element_type=F32
            )
            if p == 0:
                acc[g, half, start:stop, :] = product
            elif p < 3:
                acc[g, half, start:stop, :] = acc[g, half, start:stop, :] + product
            else:
                total = acc[g, half, start:stop, :] + product
                final[half, start:stop, :] = total
                most.append(jnp.max(total[0:592].reshape(74, 8, 256), axis=0))
                if stop - start > 592:
                    most.append(jnp.broadcast_to(jnp.max(total[592:], axis=0, keepdims=True), (8, 256)))
        if p == 3:
            if stretch == 1:
                most.append(tops[...])
            tops[...] = functools.reduce(jnp.maximum, most)

    def scaled(g):
        total = jnp.sum(jnp.transpose(squares[g]), axis=0, keepdims=True)
        scales[0:1, :] = lax.rsqrt(total / (4 * plane_width) + EPSILON)

    def peaked():
        scales[1:2, :] = jnp.max(tops[...], axis=0, keepdims=True) * scales[0:1, :]

    def folded(g, half):
        scale = jnp.broadcast_to(scales[0:1, :], (8, 256))
        peaks = jnp.broadcast_to(scales[1:2, :], (8, 256))
        sublane = lax.broadcasted_iota(jnp.int32, (8, 256), 0)
        holder = core if half == 0 else 1 - core
        first_word = (((y * 2 + holder) * 4 + x) * 4 + z) * nwords
        local = targets_v[...].reshape(1, 128) - first_word
        local = jnp.where(local < nwords, local, -8)
        local = spread(jnp.where(segment == core * GROUPS + g, local, 0))
        wanted = jnp.broadcast_to(jnp.concatenate([local, local], axis=1), (8, 256)) - sublane
        if half == 0:
            mass = moment = picked = jnp.zeros((8, 256), F32)
        else:
            mass, moment, picked = (sums[k] for k in range(3))
        for k in range(150):
            z_all = final[half, 8 * k : 8 * k + 8, :] * scale
            z_rel = z_all - peaks
            e = jnp.exp(z_rel)
            mass = mass + e
            moment = moment + e * z_rel
            picked = jnp.where(wanted == 8 * k, z_all, picked)
        if half == 0:
            for k, value in enumerate((mass, moment, picked)):
                sums[k] = value
            return
        found = [scales[1:2, :]] + [jnp.sum(v, axis=0, keepdims=True) for v in (mass, moment, picked)]
        for k, value in enumerate(found):
            stats[g, 2 * k : 2 * k + 1, :] = value[:, 0:128]
            stats[g, 2 * k + 1 : 2 * k + 2, :] = value[:, 128:256]

    def words_ready(p):
        plane = source[0][PLANES[p]]
        own_words[p].wait()
        pltpu.make_async_remote_copy(
            src_ref=unembed_hbm.at[:, columns(plane)],
            dst_ref=words.at[1, plane, pl.ds(0, nwords)],
            send_sem=words_send.at[p],
            recv_sem=words_recv.at[p],
            device_id=partner,
            device_id_type=MESH,
        ).wait_recv()

    run(PLAN[0])
    part.wait_recv()
    for zp in range(2):
        prepare(0, 0, zp, rows_c)
    run(PLAN[1])
    words_ready(0)
    multiply(0, 0, 0, rows_c)
    run(PLAN[2])
    multiply(0, 0, 1, rows_c)
    run(PLAN[3])
    for zp in range(2):
        prepare(1, 0, zp, rows_a)
    for g, now, later in ((1, rows_a, rows_b), (2, rows_b, rows_c), (3, rows_c, rows_a)):
        for k in range(2):
            run(PLAN[2 + 2 * g + k])
            multiply(g, 0, k, now)
            prepare(*((g + 1, 0) if g < 3 else (0, 1)), k, later)

    def body(g, carry):
        rotation = (rows_a, rows_b, rows_c)
        for p in (1, 2, 3):
            now, later = rotation[p - 1], rotation[p % 3]
            following = (g, p + 1) if p < 3 else (jnp.minimum(g + 1, GROUPS - 1), 1)
            former_group = lax.rem(g + GROUPS - 1, GROUPS)
            if p == 3:
                scaled(g)
            for k in range(2):
                rows_of_plan = [PLAN[10 + 6 * j + 2 * (p - 1) + k] for j in range(GROUPS)]
                dispatch(g, [functools.partial(run, row) if row else None for row in rows_of_plan])
                if k == 0:
                    pl.when(g == 0)(functools.partial(words_ready, p))
                multiply(g, p, k, now)
                prepare(*following, k, later)
                if p == 1:
                    folded(former_group, k)
            if p == 3:
                peaked()
        return carry

    lax.fori_loop(0, GROUPS, body, 0)
    run(PLAN[34])
    for half in range(2):
        folded(GROUPS - 1, half)

    def joined(parts):
        most = functools.reduce(jnp.maximum, [part[0] for part in parts])
        shifts = [part[0] - most for part in parts]
        factors = [jnp.exp(shift) for shift in shifts]
        mass = sum(f * part[1] for f, part in zip(factors, parts))
        moment = sum(f * (part[2] + shift * part[1]) for f, shift, part in zip(factors, shifts, parts))
        return most, mass, moment, sum(part[3] for part in parts)

    wide_segment = lax.broadcasted_iota(jnp.int32, (8, 128), 1) // 32
    for q in range(4):
        value = jnp.zeros((8, 128), F32)
        for g in range(GROUPS):
            shift = 32 * ((g - q) % 4)
            moved_row = pltpu.roll(stats[g], shift, 1) if shift else stats[g]
            value = jnp.where(wide_segment == g, moved_row, value)
        for half in range(2):
            for k in range(4):
                slices[half * 4 + q, k : k + 1, :] = value[2 * k + half : 2 * k + half + 1, :]

    def section_copy(step, other):
        yy = lax.rem(y + step, 4)
        cc = 1 - core if other else core
        at = step * 2 + other
        return pltpu.make_async_remote_copy(
            src_ref=slices.at[yy * 2 + cc],
            dst_ref=from_section.at[at],
            send_sem=section_send.at[at],
            recv_sem=section_recv.at[at],
            device_id=section_peer(step, other),
            device_id_type=MESH,
        )

    for p in section_peers:
        section_copy(*p).start()
    from_section[0] = slices[section]
    for p in section_peers:
        section_copy(*p).wait_recv()
    for other in range(2):
        arrived = [from_section[2 * step + other] for step in range(4)]
        found = joined([[part[k : k + 1] for k in range(4)] for part in arrived])
        for k, value in enumerate(found):
            row = 4 * (core if other == 0 else 1 - core) + k
            partial[pl.ds(row, 1), :] = value

    def plane_copy(step):
        return pltpu.make_async_remote_copy(
            src_ref=partial,
            dst_ref=from_plane.at[step],
            send_sem=plane_send.at[step],
            recv_sem=plane_recv.at[step],
            device_id=plane_peer(step),
            device_id_type=MESH,
        )

    for step in range(1, 16):
        plane_copy(step).start()
    from_plane[0] = partial[...]
    for step in range(1, 16):
        plane_copy(step).wait_recv()
    everything = [from_plane[step] for step in range(16)]
    narrow = lax.broadcasted_iota(jnp.int32, (1, 128), 1)
    result = [[jnp.zeros((1, 128), F32) for _ in range(2)] for _ in range(3)]
    for half in range(2):
        most, mass, moment, picked = joined([[part[4 * half + k : 4 * half + k + 1] for k in range(4)] for part in everything])
        log_mass = jnp.log(mass)
        lse = most + log_mass
        for n, value in enumerate((lse, log_mass - moment / mass, picked - lse)):
            for l in range(2):
                for g in range(GROUPS):
                    shift = (64 * half + 16 * g - 32 * g - 16 * l) % 128
                    moved_row = pltpu.roll(value, shift, 1) if shift else value
                    result[n][l] = jnp.where(narrow // GTOK == 4 * half + g, moved_row, result[n][l])
    for n in range(3):
        for l in range(2):
            out_ref[n, l : l + 1, :] = result[n][l]

    for p in section_peers:
        section_copy(*p).wait_send()
    for step in range(1, 16):
        plane_copy(step).wait_send()
    part.wait_send()
    for copy in their_words:
        copy.wait_send()
    for row, (dx, dy, dz, link) in enumerate(TREE):
        if dy == 0:
            gain_copy(parent((dx, dy, dz), link), link).wait_send()
    for g in range(GROUPS):
        pltpu.make_async_remote_copy(
            src_ref=gat.at[pl.ds(0, len(TREE))],
            dst_ref=gat.at[pl.ds(0, len(TREE))],
            send_sem=send_sem.at[g],
            recv_sem=recv_sem.at[0],
            device_id=neighbours[0],
            device_id_type=MESH,
        ).wait_send()


def wrapped(c):
    return (c + 1) % 4 - 1


def parent(n, link):
    axis, way = LINKS[link]
    n = list(n)
    n[axis] = wrapped(n[axis] - way)
    return tuple(n)


def child(n, link):
    axis, way = LINKS[link]
    n = list(n)
    n[axis] = wrapped(n[axis] + way)
    return tuple(n)


TREE_INDEX = {row[:3]: k for k, row in enumerate(TREE)}
GAIN_INDEX = {k: i for i, k in enumerate(k for k, row in enumerate(TREE) if row[1] == 0)}


def shards(stream_in, deltas, norm_gain, unembed, targets):
    nwords, width = unembed.shape
    anywhere = pl.BlockSpec(memory_space=pl.ANY)
    inside = pl.BlockSpec(memory_space=pltpu.VMEM)
    dma = pltpu.SemaphoreType.DMA
    out = pl.pallas_call(
        kernel,
        out_shape=jax.ShapeDtypeStruct((3, 2, 128), F32),
        in_specs=[anywhere] * 5,
        out_specs=inside,
        scratch_shapes=[
            pltpu.VMEM((320, 128), BF16),
            pltpu.VMEM((2, 320, 128), BF16),
            pltpu.VMEM((128,), jnp.int32),
            pltpu.VMEM((320,), F32),
            pltpu.VMEM((16, 8, 128), F32),
            pltpu.VMEM((GROUPS, 5, GTOK, 128), BF16),
            pltpu.VMEM((64 * GROUPS, 2, 5, GTOK, 128), BF16),
            pltpu.VMEM((2, 4, nwords, width // 4), BF16),
            pltpu.VMEM((256, width // 4), BF16),
            pltpu.VMEM((256, width // 4), BF16),
            pltpu.VMEM((256, width // 4), BF16),
            pltpu.VMEM((GROUPS, 2, 1200, 256), F32),
            pltpu.VMEM((2, 1200, 256), F32),
            pltpu.VMEM((GROUPS, 256, 128), F32),
            pltpu.VMEM((8, 256), F32),
            pltpu.VMEM((8, 256), F32),
            pltpu.VMEM((3, 8, 256), F32),
            pltpu.VMEM((GROUPS, 8, 128), F32),
            pltpu.VMEM((8, 4, 128), F32),
            pltpu.VMEM((8, 4, 128), F32),
            pltpu.VMEM((8, 128), F32),
            pltpu.VMEM((16, 8, 128), F32),
            dma((4,)),
            dma((4,)),
            dma((4,)),
            dma((4,)),
            dma((15,)),
            dma((15,)),
            dma,
            dma,
            dma((GROUPS,)),
            dma((63 * GROUPS,)),
            dma((8,)),
            dma((8,)),
            dma((16,)),
            dma((16,)),
        ],
        compiler_params=pltpu.CompilerParams(
            collective_id=0, has_side_effects=True, vmem_limit_bytes=60 * 1024 * 1024
        ),
    )(stream_in.T, deltas.transpose(0, 2, 1), norm_gain, unembed, targets)
    return out[0], out[1], out[2]


def solution(mesh):
    torus = Mesh(
        mesh.devices.reshape(mesh.shape["section"], 4, 4), ("section", "vocab_0", "vocab_1")
    )
    placed = (P(None, VOCAB), P("section", None, VOCAB), P(VOCAB), P(SECTION_VOCAB, None), P())
    return jax.shard_map(
        shards,
        mesh=torus,
        in_specs=placed,
        out_specs=(P("section", None), P("section", None), P("section", None)),
        check_vma=False,
    )
```

```python
import functools

import jax
import jax.numpy as jnp
from jax import lax
from jax.experimental import pallas as pl
from jax.experimental.pallas import tpu as pltpu
from jax.sharding import Mesh
from jax.sharding import PartitionSpec as P

MESH = pl.DeviceIdType.MESH
F32 = jnp.float32
BF16 = jnp.bfloat16
EPSILON = 1e-06

VOCAB = ("vocab_0", "vocab_1")
SECTION_VOCAB = ("section", "vocab_0", "vocab_1")

LINKS = ((0, 1), (0, -1), (1, 1), (1, -1), (2, 1), (2, -1))
TREE = (
    (-1, 0, 0, 1), (0, -1, 0, 3), (0, 0, -1, 5), (0, 0, 1, 4), (0, 1, 0, 2), (1, 0, 0, 0),
    (-1, -1, 0, 3), (-1, 0, -1, 1), (-1, 0, 1, 1), (-1, 1, 0, 1), (0, -1, -1, 5), (0, -1, 1, 4),
    (0, 0, 2, 4), (0, 1, -1, 5), (0, 1, 1, 2), (0, 2, 0, 2), (1, -1, 0, 0), (1, 0, -1, 0),
    (1, 0, 1, 0), (1, 1, 0, 0), (2, 0, 0, 0), (-1, -1, -1, 3), (-1, -1, 1, 1), (-1, 0, 2, 5),
    (-1, 1, -1, 5), (-1, 1, 1, 2), (-1, 2, 0, 1), (0, -1, 2, 3), (0, 1, 2, 4), (0, 2, -1, 3),
    (0, 2, 1, 2), (1, -1, -1, 0), (1, -1, 1, 4), (1, 0, 2, 4), (1, 1, -1, 2), (1, 1, 1, 2),
    (1, 2, 0, 3), (2, -1, 0, 0), (2, 0, -1, 0), (2, 0, 1, 1), (2, 1, 0, 2), (-1, -1, 2, 4),
    (-1, 1, 2, 5), (-1, 2, -1, 5), (-1, 2, 1, 3), (0, 2, 2, 5), (1, -1, 2, 5), (1, 1, 2, 4),
    (1, 2, -1, 3), (1, 2, 1, 3), (2, -1, -1, 0), (2, -1, 1, 1), (2, 0, 2, 5), (2, 1, -1, 2),
    (2, 1, 1, 2), (2, 2, 0, 3), (-1, 2, 2, 4), (1, 2, 2, 4), (2, -1, 2, 3), (2, 1, 2, 5),
    (2, 2, -1, 2), (2, 2, 1, 1), (2, 2, 2, 1),
)
PLAN = (
    (
        (1, 0, 0), (1, 1, 0), (1, 2, 0), (1, 3, 0), (1, 4, 0), (1, 5, 0), (1, 0, 1), (1, 1, 1), (1, 2, 1),
        (1, 3, 1), (1, 4, 1), (1, 5, 1), (1, 0, 2), (1, 1, 2), (1, 2, 2), (1, 3, 2), (1, 4, 2), (1, 5, 2),
        (1, 0, 3), (1, 1, 3), (1, 2, 3), (1, 3, 3), (1, 4, 3), (1, 5, 3), (0, 0, 0), (0, 1, 0), (0, 2, 0),
        (0, 3, 0), (0, 4, 0), (0, 5, 0), (1, 6, 0), (1, 8, 0), (1, 10, 0), (1, 11, 0), (1, 15, 0), (1, 16, 0),
        (1, 9, 0), (1, 17, 0), (0, 0, 1), (0, 1, 1), (0, 2, 1), (0, 3, 1), (0, 4, 1), (0, 5, 1), (1, 6, 1),
        (1, 10, 1), (1, 11, 1), (1, 15, 1), (1, 7, 0), (1, 18, 0), (0, 0, 2), (0, 1, 2), (0, 2, 2), (0, 3, 2),
        (0, 4, 2), (0, 5, 2), (1, 6, 2), (1, 10, 2), (1, 11, 2), (1, 15, 2), (1, 8, 1), (1, 16, 1), (0, 0, 3),
        (0, 1, 3), (0, 2, 3), (0, 3, 3), (0, 4, 3), (0, 5, 3), (1, 6, 3), (1, 10, 3), (1, 11, 3), (1, 15, 3),
        (1, 9, 1), (1, 12, 0), (1, 13, 0), (1, 14, 0), (1, 17, 1), (1, 13, 1), (1, 14, 1), (0, 6, 0), (0, 8, 0),
        (0, 10, 0), (0, 11, 0), (0, 15, 0), (0, 16, 0), (1, 22, 0), (1, 29, 0), (1, 31, 0), (1, 32, 0), (1, 12, 1),
        (1, 13, 2), (1, 14, 2), (0, 6, 1), (0, 9, 0), (0, 10, 1), (0, 11, 1), (0, 15, 1), (0, 17, 0), (1, 22, 1),
        (1, 29, 1), (1, 38, 0), (1, 24, 0), (1, 26, 0), (1, 12, 2), (1, 14, 3), (1, 18, 1), (0, 6, 2), (0, 7, 0),
        (0, 10, 2), (0, 11, 2), (0, 15, 2), (0, 18, 0), (1, 29, 2), (1, 12, 3), (1, 13, 3), (1, 16, 2), (1, 35, 0),
        (1, 39, 0), (0, 6, 3), (0, 8, 1), (0, 10, 3), (0, 11, 3), (0, 15, 3), (0, 16, 1), (1, 29, 3), (1, 22, 2),
        (1, 17, 2), (0, 9, 1), (0, 12, 0), (0, 13, 0), (0, 14, 0), (0, 17, 1), (1, 27, 0), (1, 28, 0), (1, 30, 0),
        (0, 29, 0), (1, 45, 0), (1, 7, 1), (1, 32, 1), (1, 19, 0), (0, 22, 0), (0, 13, 1), (0, 14, 1), (0, 31, 0),
        (0, 32, 0), (1, 44, 0), (1, 30, 1), (1, 49, 0), (0, 29, 1), (1, 45, 1), (1, 26, 1), (1, 28, 1), (1, 20, 0),
        (0, 22, 1), (0, 12, 1), (0, 13, 2), (0, 14, 2), (0, 38, 0), (1, 30, 2), (1, 27, 1), (0, 29, 2), (1, 45, 2),
        (1, 28, 2), (1, 37, 0), (1, 51, 0), (0, 24, 0), (0, 26, 0), (0, 12, 2), (0, 14, 3), (0, 18, 1), (1, 30, 3),
        (1, 27, 2), (0, 29, 3), (1, 45, 3), (1, 8, 2), (1, 28, 3), (1, 46, 0), (1, 38, 1), (1, 53, 0), (0, 12, 3),
        (0, 13, 3), (0, 16, 2), (0, 35, 0), (0, 39, 0), (1, 27, 3), (0, 27, 0), (1, 31, 1), (1, 34, 0), (1, 52, 0),
        (0, 22, 2), (0, 28, 0), (0, 30, 0), (0, 45, 0), (0, 17, 2),
    ),
    (
        (1, 44, 1), (0, 44, 0), (1, 56, 0), (1, 61, 0),
    ),
    (
        (1, 23, 0), (1, 9, 2), (1, 18, 2), (1, 35, 1), (1, 47, 0), (0, 7, 1), (0, 30, 1), (0, 45, 1), (0, 32, 1),
        (0, 19, 0), (1, 48, 0), (0, 49, 0),
    ),
    (
        (1, 25, 0), (1, 43, 0), (1, 16, 3), (1, 57, 0), (1, 39, 1), (0, 26, 1), (0, 28, 1), (0, 30, 2), (0, 45, 2),
        (0, 20, 0), (1, 36, 0), (0, 27, 1),
    ),
    (
        (1, 22, 3), (1, 42, 0), (1, 17, 3), (1, 33, 0), (1, 54, 0), (0, 28, 2), (0, 30, 3), (0, 45, 3), (0, 37, 0),
        (0, 51, 0), (1, 49, 1), (0, 27, 2),
    ),
    (
        (1, 41, 0), (1, 7, 2), (1, 24, 1), (1, 50, 0), (0, 8, 2), (0, 28, 3), (0, 46, 0), (0, 38, 1), (0, 53, 0),
        (1, 60, 0), (1, 21, 0), (0, 27, 3),
    ),
    (
        (1, 32, 2), (1, 19, 1), (1, 40, 0), (1, 59, 0), (0, 56, 0), (0, 31, 1), (0, 34, 0), (0, 52, 0), (0, 61, 0),
        (1, 62, 0), (1, 58, 0), (0, 44, 1),
    ),
    (
        (1, 26, 2), (1, 56, 1), (1, 46, 1), (1, 20, 1), (1, 53, 1), (0, 23, 0), (0, 9, 2), (0, 18, 2), (0, 35, 1),
        (0, 47, 0), (1, 55, 0), (0, 48, 0),
    ),
    (
        (1, 34, 1), (1, 47, 1), (1, 37, 1), (1, 51, 1), (1, 52, 1), (0, 25, 0), (0, 43, 0), (0, 16, 3), (0, 57, 0),
        (0, 39, 1), (1, 44, 2), (0, 36, 0), (1, 23, 1), (1, 35, 2), (1, 38, 2), (1, 61, 1), (0, 22, 3), (0, 42, 0),
        (0, 17, 3), (0, 33, 0), (0, 54, 0),
    ),
    (
        (1, 48, 1), (0, 49, 1), (1, 57, 1), (1, 8, 3), (1, 25, 1), (1, 43, 1), (1, 31, 2), (1, 33, 1), (0, 41, 0),
        (0, 7, 2), (0, 24, 1), (0, 50, 0), (0, 60, 0),
    ),
    (
        (1, 36, 1), (0, 21, 0), (1, 41, 1), (1, 9, 3), (1, 42, 1), (1, 18, 3), (1, 54, 1), (0, 32, 2), (0, 19, 1),
        (0, 40, 0), (0, 59, 0), (0, 62, 0), (1, 49, 2),
    ),
    (
        (0, 58, 0), (1, 24, 2), (1, 32, 3), (1, 50, 1), (0, 26, 2), (0, 56, 1), (0, 46, 1), (0, 20, 1), (0, 53, 1),
        (1, 60, 1), (1, 62, 1), (1, 21, 1), (0, 55, 0),
    ),
    (
        (1, 19, 2), (1, 39, 2), (1, 40, 1), (1, 59, 1), (0, 34, 1), (0, 47, 1), (0, 37, 1), (0, 51, 1), (0, 52, 1),
        (1, 58, 1), (0, 44, 2), (1, 56, 2),
    ),
    (
        (1, 7, 3), (1, 20, 2), (0, 23, 1), (0, 35, 2), (0, 57, 1), (0, 38, 2), (0, 61, 1), (1, 47, 2), (1, 52, 2),
        (1, 53, 2), (1, 55, 1), (0, 48, 1),
    ),
    (
        (1, 26, 3), (1, 33, 2), (1, 34, 2), (1, 37, 2), (0, 8, 3), (0, 25, 1), (0, 43, 1), (0, 31, 2), (0, 33, 1),
        (1, 46, 2), (1, 44, 3), (0, 36, 1),
    ),
    (
        (1, 23, 2), (1, 51, 2), (1, 38, 3), (0, 41, 1), (0, 9, 3), (0, 42, 1), (0, 18, 3), (0, 54, 1), (1, 35, 3),
        (1, 48, 2), (0, 49, 2), (1, 57, 2),
    ),
    (
        (1, 41, 2), (1, 25, 2), (1, 43, 2), (1, 31, 3), (1, 61, 2), (0, 24, 2), (0, 32, 3), (0, 50, 1), (0, 60, 1),
        (0, 62, 1), (1, 36, 2), (0, 21, 1),
    ),
    (
        (1, 42, 2), (1, 33, 3), (1, 50, 2), (0, 56, 2), (0, 19, 2), (0, 39, 2), (0, 40, 1), (0, 59, 1), (1, 54, 2),
        (1, 62, 2), (1, 49, 3), (0, 58, 1),
    ),
    (
        (1, 41, 3), (1, 24, 3), (1, 19, 3), (1, 39, 3), (0, 7, 3), (0, 47, 2), (0, 20, 2), (0, 52, 2), (0, 53, 2),
        (1, 60, 2), (1, 21, 2), (0, 55, 1), (1, 51, 3), (1, 20, 3), (1, 40, 2), (1, 59, 2),
    ),
    (
        (0, 26, 3), (0, 46, 2), (0, 33, 2), (0, 34, 2), (0, 37, 2), (1, 58, 2), (0, 44, 3), (1, 56, 3), (1, 37, 3),
        (1, 61, 3), (0, 23, 2), (0, 35, 3), (0, 57, 2), (0, 51, 2), (0, 38, 3),
    ),
    (
        (1, 47, 3), (1, 52, 3), (1, 53, 3), (1, 55, 2), (0, 48, 2), (1, 34, 3), (0, 41, 2), (0, 25, 2), (0, 43, 2),
        (0, 31, 3), (0, 61, 2), (1, 46, 3), (1, 50, 3), (1, 48, 3), (0, 36, 2),
    ),
    (
        (1, 23, 3), (1, 25, 3), (0, 42, 2), (0, 33, 3), (0, 50, 2), (0, 54, 2), (0, 62, 2), (1, 36, 3), (0, 49, 3),
        (1, 57, 3),
    ),
    (
        (1, 43, 3), (0, 41, 3), (0, 24, 3), (0, 19, 3), (0, 39, 3), (0, 60, 2), (1, 54, 3), (1, 21, 3), (0, 21, 2),
    ),
    (
        (1, 42, 3), (0, 56, 3), (0, 51, 3), (0, 20, 3), (0, 40, 2), (0, 59, 2), (1, 40, 3), (1, 62, 3), (0, 58, 2),
    ),
    (
        (0, 47, 3), (0, 37, 3), (0, 52, 3), (0, 53, 3), (0, 61, 3), (1, 58, 3), (1, 59, 3), (1, 60, 3), (1, 55, 3),
        (0, 55, 2),
    ),
    (
        (0, 46, 3), (0, 34, 3), (0, 50, 3), (0, 48, 3), (0, 57, 3),
    ),
    (
        (0, 23, 3), (0, 25, 3), (0, 36, 3),
    ),
    (
        (0, 43, 3), (0, 54, 3), (0, 21, 3), (0, 62, 3),
    ),
    (
        (0, 42, 3), (0, 40, 3), (0, 58, 3),
    ),
    (
        (0, 59, 3), (0, 60, 3), (0, 55, 3),
    ),
    (),
    (),
    (),
    (),
    (),
)
PLANES = (0, 1, -1, 2)

GROUPS = 4
GTOK = 16
FILL = -1e30


def dispatch(index, branches, low=0, high=None):
    high = len(branches) if high is None else high
    if not any(branches[low:high]):
        return
    if high - low == 1:
        branches[low]()
        return
    mid = (low + high) // 2

    @pl.when(index < mid)
    def _():
        dispatch(index, branches, low, mid)

    @pl.when(index >= mid)
    def _():
        dispatch(index, branches, mid, high)


def kernel(
    stream_hbm, deltas_hbm, gain_hbm, unembed_hbm, targets_hbm, out_ref,
    stream_v, deltas_v, targets_v, gain_v, gains, outbox, gat, words, rows_a, rows_b, rows_c, acc, final,
    squares, scales, tops, sums, stats, slices, from_section, partial, from_plane,
    load_sem, own_sem, words_send, words_recv, gain_send, gain_recv,
    part_send, part_recv, send_sem, recv_sem,
    section_send, section_recv, plane_send, plane_recv,
):
    section = lax.axis_index("section")
    x = lax.axis_index("vocab_0")
    z = lax.axis_index("vocab_1")
    y = section // 2
    core = section % 2
    sign = 1 - 2 * core
    nwords = unembed_hbm.shape[0]
    plane_width = unembed_hbm.shape[1] // 4
    home = (x, y, z)

    def device(xx, yy, zz, cc):
        return (yy * 2 + cc, xx, zz)

    def moved(axis, step):
        at = list(home)
        at[axis] = lax.rem(at[axis] + step + 4, 4)
        return tuple(at)

    neighbours = [device(*moved(axis, way * sign), core) for axis, way in LINKS]
    partner = device(x, y, z, 1 - core)
    source = [{d: lax.rem(home[axis] - sign * d + 4, 4) for d in (-1, 0, 1, 2)} for axis in range(3)]

    loads = [
        pltpu.make_async_copy(stream_hbm, stream_v, load_sem.at[0]),
        pltpu.make_async_copy(deltas_hbm, deltas_v, load_sem.at[1]),
        pltpu.make_async_copy(targets_hbm, targets_v, load_sem.at[2]),
        pltpu.make_async_copy(gain_hbm, gain_v, load_sem.at[3]),
    ]
    for copy in loads:
        copy.start()

    def plane_peer(step):
        return device(lax.rem(x + step // 4, 4), y, lax.rem(z + step % 4, 4), core)

    def section_peer(step, other):
        return device(x, lax.rem(y + step, 4), z, 1 - core if other else core)

    section_peers = [(step, other) for step in range(4) for other in (0, 1) if step or other]
    barrier = pltpu.get_barrier_semaphore()
    around = [device(*moved(axis, way), cc) for axis, way in LINKS for cc in range(2)]
    for peer in around + [partner]:
        pl.semaphore_signal(barrier, inc=1, device_id=peer, device_id_type=MESH)

    def columns(plane):
        return pl.ds(pl.multiple_of(plane * plane_width, 128), plane_width)

    own_words = []
    for p, dx in enumerate(PLANES):
        plane = source[0][dx]
        own_words.append(
            pltpu.make_async_copy(
                unembed_hbm.at[:, columns(plane)], words.at[0, plane, pl.ds(0, nwords)], own_sem.at[p]
            )
        )
        own_words[-1].start()

    for copy in loads:
        copy.wait()

    lane = lax.broadcasted_iota(jnp.int32, (GTOK, 128), 1)
    low = lane < 64
    odd = lax.rem(z, 2) == 1
    my_slot = ((x * 4 + y) * 4 + z) * GROUPS

    first = jnp.where(section == 0, 1.0, 0.0).astype(F32)
    former = deltas_v[0].astype(F32) + stream_v[...].astype(F32) * first
    kept = former.astype(BF16).astype(F32)
    latter = deltas_v[1].astype(F32) + (former - kept)
    packed = []
    heads = []
    for value in (kept, latter):
        packed.append(jnp.where(odd, value[64:192], value[0:128]))
        packed.append(jnp.where(odd, value[192:320], value[128:256]))
        heads.append(jnp.where(odd, value[0:64], value[256:320]))
    lead = jnp.where(odd, heads[1], heads[0])
    trail = jnp.where(odd, heads[0], heads[1])
    packed.append(jnp.concatenate([lead, trail], axis=0))
    for k, value in enumerate(packed):
        tile = jnp.transpose(value).astype(BF16)
        for half in range(2):

            @pl.when(core == half)
            def _():
                for g in range(GROUPS):
                    t0 = half * 64 + g * GTOK
                    gat[my_slot + g, core, k] = tile[t0 : t0 + GTOK]

            @pl.when(core != half)
            def _():
                for g in range(GROUPS):
                    t0 = half * 64 + g * GTOK
                    outbox[g, k] = tile[t0 : t0 + GTOK]

    low_row = lax.broadcasted_iota(jnp.int32, (1, 128), 1) < 64
    none = jnp.zeros((1, 64), F32)
    g0 = gain_v[0:128].reshape(1, 128)
    g1 = gain_v[128:256].reshape(1, 128)
    g2 = jnp.concatenate([gain_v[256:320].reshape(1, 64), none], axis=1)
    t0, t1, t2 = (pltpu.roll(v, 64, 1) for v in (g0, g1, g2))
    blank = jnp.zeros((1, 128), F32)
    gain_rows = (
        (g0, blank),
        (g1, blank),
        (g2, jnp.where(low_row, 0.0, t0)),
        (blank, jnp.where(low_row, t0, t1)),
        (blank, jnp.where(low_row, t1, t2)),
    )
    gains[x * 4 + z] = jnp.concatenate(
        [jnp.where(odd, other, even) for even, other in gain_rows] + [blank] * 3, axis=0
    )

    final[:, 1184:1200, :] = jnp.full((2, 16, 256), FILL, F32)

    pl.semaphore_wait(barrier, 13)

    part = pltpu.make_async_remote_copy(
        src_ref=outbox,
        dst_ref=gat.at[pl.ds(my_slot, GROUPS), core],
        send_sem=part_send,
        recv_sem=part_recv,
        device_id=partner,
        device_id_type=MESH,
    )
    part.start()

    def gain_copy(n, link):
        at = (source[0][n[0]] * 4 + source[2][n[2]])
        place = (TREE_INDEX[child(n, link)] if link is not None else TREE_INDEX[n])
        return pltpu.make_async_remote_copy(
            src_ref=gains.at[at],
            dst_ref=gains.at[at],
            send_sem=gain_send.at[GAIN_INDEX[place]],
            recv_sem=gain_recv.at[GAIN_INDEX[place]],
            device_id=neighbours[link or 0],
            device_id_type=MESH,
        )

    def block_copy(n, row, link, g):
        slot = source[0][n[0]] * 64 + source[1][n[1]] * 16 + source[2][n[2]] * 4 + g
        return pltpu.make_async_remote_copy(
            src_ref=gat.at[slot],
            dst_ref=gat.at[slot],
            send_sem=send_sem.at[g],
            recv_sem=recv_sem.at[row * GROUPS + g],
            device_id=neighbours[link],
            device_id_type=MESH,
        )

    def first_copy(row, link, g, away):
        axis, way = LINKS[link]
        return pltpu.make_async_remote_copy(
            src_ref=outbox.at[g] if away else gat.at[my_slot + g, core],
            dst_ref=gat.at[my_slot + g, core],
            send_sem=send_sem.at[g],
            recv_sem=recv_sem.at[row * GROUPS + g],
            device_id=device(*moved(axis, -way * sign), 1 - core) if away else neighbours[link],
            device_id_type=MESH,
        )

    def send_gain(n):
        for row, (dx, dy, dz, link) in enumerate(TREE):
            if dy == 0 and parent((dx, dy, dz), link) == n:
                gain_copy(n, link).start()

    def run(actions):
        for kind, row, g in actions:
            dx, dy, dz, link = TREE[row]
            n = (dx, dy, dz)
            if kind == 0:
                block_copy(n, row, link, g).wait_recv()
                if g == 0 and dy == 0:
                    gain_copy(n, None).wait_recv()
                    send_gain(n)
            elif parent(n, link) == (0, 0, 0):
                for away in (False, True):
                    first_copy(row, link, g, away).start()
            else:
                block_copy(parent(n, link), row, link, g).start()

    send_gain((0, 0, 0))

    their_words = []
    for p, dx in enumerate(PLANES):
        plane = lax.rem(x + sign * dx + 4, 4)
        their_words.append(
            pltpu.make_async_remote_copy(
                src_ref=unembed_hbm.at[:, columns(plane)],
                dst_ref=words.at[1, plane, pl.ds(0, nwords)],
                send_sem=words_send.at[p],
                recv_sem=words_recv.at[p],
                device_id=partner,
                device_id_type=MESH,
            )
        )

    for copy in their_words:
        copy.start()

    segment = lax.broadcasted_iota(jnp.int32, (1, 128), 1) // GTOK

    def spread(value):
        for step in (16, 32, 64):
            value = value + pltpu.roll(value, step, 1)
        return value

    def prepare(g, p, zp, rows):
        plane = source[0][PLANES[p]]
        running = [jnp.zeros((GTOK, 128), F32) for _ in range(5)]
        both = gains[plane * 4 + 2 * zp] + gains[plane * 4 + 2 * zp + 1]
        factor = [jnp.broadcast_to(both[k : k + 1, :], (GTOK, 128)) for k in range(5)]
        for yy in range(4):
            even = plane * 64 + yy * 16 + 2 * zp * 4 + g
            other = even + 4
            for cc in range(2):
                pe = gat[even, cc, 4].astype(F32)
                po = gat[other, cc, 4].astype(F32)
                for l in range(2):
                    layer = 4 * yy + 2 * cc + l
                    if l == 0:
                        middle = jnp.where(low, pe, po)
                    else:
                        middle = pltpu.roll(jnp.where(low, po, pe), 64, 1)
                    values = [
                        gat[even, cc, 2 * l].astype(F32),
                        gat[even, cc, 2 * l + 1].astype(F32),
                        middle,
                        gat[other, cc, 2 * l].astype(F32),
                        gat[other, cc, 2 * l + 1].astype(F32),
                    ]
                    span = slice(layer * GTOK, (layer + 1) * GTOK)
                    total = jnp.zeros((GTOK, 128), F32) if p == 0 and zp == 0 else squares[g, span, :]
                    for k in range(5):
                        at = 5 * zp + k
                        running[k] = running[k] + values[k]
                        total = total + running[k] * running[k]
                        rows[span, at * 128 : (at + 1) * 128] = (running[k] * factor[k]).astype(BF16)
                    squares[g, span, :] = total

    def multiply(g, p, stretch, rows):
        start, stop = ((0, 592), (592, nwords))[stretch]
        plane = source[0][PLANES[p]]
        most = []
        for half in range(2):
            product = lax.dot_general(
                words[half, plane, start:stop, :], rows[...], (((1,), (1,)), ((), ())), preferred_element_type=F32
            )
            if p == 0:
                acc[g, half, start:stop, :] = product
            elif p < 3:
                acc[g, half, start:stop, :] = acc[g, half, start:stop, :] + product
            else:
                total = acc[g, half, start:stop, :] + product
                final[half, start:stop, :] = total
                most.append(jnp.max(total[0:592].reshape(74, 8, 256), axis=0))
                if stop - start > 592:
                    most.append(jnp.broadcast_to(jnp.max(total[592:], axis=0, keepdims=True), (8, 256)))
        if p == 3:
            if stretch == 1:
                most.append(tops[...])
            tops[...] = functools.reduce(jnp.maximum, most)

    def scaled(g):
        total = jnp.sum(jnp.transpose(squares[g]), axis=0, keepdims=True)
        scales[0:1, :] = lax.rsqrt(total / (4 * plane_width) + EPSILON)

    def peaked():
        scales[1:2, :] = jnp.max(tops[...], axis=0, keepdims=True) * scales[0:1, :]

    def folded(g, piece):
        half = piece // 2
        scale = jnp.broadcast_to(scales[0:1, :], (8, 256))
        peaks = jnp.broadcast_to(scales[1:2, :], (8, 256))
        sublane = lax.broadcasted_iota(jnp.int32, (8, 256), 0)
        holder = core if half == 0 else 1 - core
        first_word = (((y * 2 + holder) * 4 + x) * 4 + z) * nwords
        local = targets_v[...].reshape(1, 128) - first_word
        local = jnp.where(local < nwords, local, -8)
        local = spread(jnp.where(segment == core * GROUPS + g, local, 0))
        wanted = jnp.broadcast_to(jnp.concatenate([local, local], axis=1), (8, 256)) - sublane
        if piece == 0:
            mass = moment = picked = jnp.zeros((8, 256), F32)
        else:
            mass, moment, picked = (sums[k] for k in range(3))
        for k in range(75 * (piece % 2), 75 * (piece % 2) + 75):
            z_all = final[half, 8 * k : 8 * k + 8, :] * scale
            z_rel = z_all - peaks
            e = jnp.exp(z_rel)
            mass = mass + e
            moment = moment + e * z_rel
            picked = jnp.where(wanted == 8 * k, z_all, picked)
        if piece < 3:
            for k, value in enumerate((mass, moment, picked)):
                sums[k] = value
            return
        found = [scales[1:2, :]] + [jnp.sum(v, axis=0, keepdims=True) for v in (mass, moment, picked)]
        for k, value in enumerate(found):
            stats[g, 2 * k : 2 * k + 1, :] = value[:, 0:128]
            stats[g, 2 * k + 1 : 2 * k + 2, :] = value[:, 128:256]

    def words_ready(p):
        plane = source[0][PLANES[p]]
        own_words[p].wait()
        pltpu.make_async_remote_copy(
            src_ref=unembed_hbm.at[:, columns(plane)],
            dst_ref=words.at[1, plane, pl.ds(0, nwords)],
            send_sem=words_send.at[p],
            recv_sem=words_recv.at[p],
            device_id=partner,
            device_id_type=MESH,
        ).wait_recv()

    run(PLAN[0])
    part.wait_recv()
    for zp in range(2):
        prepare(0, 0, zp, rows_c)
    run(PLAN[1])
    words_ready(0)
    multiply(0, 0, 0, rows_c)
    run(PLAN[2])
    multiply(0, 0, 1, rows_c)
    run(PLAN[3])
    for zp in range(2):
        prepare(1, 0, zp, rows_a)
    for g, now, later in ((1, rows_a, rows_b), (2, rows_b, rows_c), (3, rows_c, rows_a)):
        for k in range(2):
            run(PLAN[2 + 2 * g + k])
            multiply(g, 0, k, now)
            prepare(*((g + 1, 0) if g < 3 else (0, 1)), k, later)

    def body(g, carry):
        rotation = (rows_a, rows_b, rows_c)
        for p in (1, 2, 3):
            now, later = rotation[p - 1], rotation[p % 3]
            following = (g, p + 1) if p < 3 else (jnp.minimum(g + 1, GROUPS - 1), 1)
            former_group = lax.rem(g + GROUPS - 1, GROUPS)
            if p == 3:
                scaled(g)
            for k in range(2):
                rows_of_plan = [PLAN[10 + 6 * j + 2 * (p - 1) + k] for j in range(GROUPS)]
                dispatch(g, [functools.partial(run, row) if row else None for row in rows_of_plan])
                if k == 0:
                    pl.when(g == 0)(functools.partial(words_ready, p))
                multiply(g, p, k, now)
                prepare(*following, k, later)
                if p < 3:
                    folded(former_group, 2 * (p - 1) + k)
            if p == 3:
                peaked()
        return carry

    lax.fori_loop(0, GROUPS, body, 0)
    run(PLAN[34])
    for piece in range(4):
        folded(GROUPS - 1, piece)

    def joined(parts):
        most = functools.reduce(jnp.maximum, [part[0] for part in parts])
        shifts = [part[0] - most for part in parts]
        factors = [jnp.exp(shift) for shift in shifts]
        mass = sum(f * part[1] for f, part in zip(factors, parts))
        moment = sum(f * (part[2] + shift * part[1]) for f, shift, part in zip(factors, shifts, parts))
        return most, mass, moment, sum(part[3] for part in parts)

    wide_segment = lax.broadcasted_iota(jnp.int32, (8, 128), 1) // 32
    for q in range(4):
        value = jnp.zeros((8, 128), F32)
        for g in range(GROUPS):
            shift = 32 * ((g - q) % 4)
            moved_row = pltpu.roll(stats[g], shift, 1) if shift else stats[g]
            value = jnp.where(wide_segment == g, moved_row, value)
        for half in range(2):
            for k in range(4):
                slices[half * 4 + q, k : k + 1, :] = value[2 * k + half : 2 * k + half + 1, :]

    def section_copy(step, other):
        yy = lax.rem(y + step, 4)
        cc = 1 - core if other else core
        at = step * 2 + other
        return pltpu.make_async_remote_copy(
            src_ref=slices.at[yy * 2 + cc],
            dst_ref=from_section.at[at],
            send_sem=section_send.at[at],
            recv_sem=section_recv.at[at],
            device_id=section_peer(step, other),
            device_id_type=MESH,
        )

    for p in section_peers:
        section_copy(*p).start()
    from_section[0] = slices[section]
    for p in section_peers:
        section_copy(*p).wait_recv()
    for other in range(2):
        arrived = [from_section[2 * step + other] for step in range(4)]
        found = joined([[part[k : k + 1] for k in range(4)] for part in arrived])
        for k, value in enumerate(found):
            row = 4 * (core if other == 0 else 1 - core) + k
            partial[pl.ds(row, 1), :] = value

    def plane_copy(step):
        return pltpu.make_async_remote_copy(
            src_ref=partial,
            dst_ref=from_plane.at[step],
            send_sem=plane_send.at[step],
            recv_sem=plane_recv.at[step],
            device_id=plane_peer(step),
            device_id_type=MESH,
        )

    for step in range(1, 16):
        plane_copy(step).start()
    from_plane[0] = partial[...]
    for step in range(1, 16):
        plane_copy(step).wait_recv()
    everything = [from_plane[step] for step in range(16)]
    narrow = lax.broadcasted_iota(jnp.int32, (1, 128), 1)
    result = [[jnp.zeros((1, 128), F32) for _ in range(2)] for _ in range(3)]
    for half in range(2):
        most, mass, moment, picked = joined([[part[4 * half + k : 4 * half + k + 1] for k in range(4)] for part in everything])
        log_mass = jnp.log(mass)
        lse = most + log_mass
        for n, value in enumerate((lse, log_mass - moment / mass, picked - lse)):
            for l in range(2):
                for g in range(GROUPS):
                    shift = (64 * half + 16 * g - 32 * g - 16 * l) % 128
                    moved_row = pltpu.roll(value, shift, 1) if shift else value
                    result[n][l] = jnp.where(narrow // GTOK == 4 * half + g, moved_row, result[n][l])
    for n in range(3):
        for l in range(2):
            out_ref[n, l : l + 1, :] = result[n][l]

    for p in section_peers:
        section_copy(*p).wait_send()
    for step in range(1, 16):
        plane_copy(step).wait_send()
    part.wait_send()
    for copy in their_words:
        copy.wait_send()
    for row, (dx, dy, dz, link) in enumerate(TREE):
        if dy == 0:
            gain_copy(parent((dx, dy, dz), link), link).wait_send()
    for g in range(GROUPS):
        pltpu.make_async_remote_copy(
            src_ref=gat.at[pl.ds(0, len(TREE))],
            dst_ref=gat.at[pl.ds(0, len(TREE))],
            send_sem=send_sem.at[g],
            recv_sem=recv_sem.at[0],
            device_id=neighbours[0],
            device_id_type=MESH,
        ).wait_send()


def wrapped(c):
    return (c + 1) % 4 - 1


def parent(n, link):
    axis, way = LINKS[link]
    n = list(n)
    n[axis] = wrapped(n[axis] - way)
    return tuple(n)


def child(n, link):
    axis, way = LINKS[link]
    n = list(n)
    n[axis] = wrapped(n[axis] + way)
    return tuple(n)


TREE_INDEX = {row[:3]: k for k, row in enumerate(TREE)}
GAIN_INDEX = {k: i for i, k in enumerate(k for k, row in enumerate(TREE) if row[1] == 0)}


def shards(stream_in, deltas, norm_gain, unembed, targets):
    nwords, width = unembed.shape
    anywhere = pl.BlockSpec(memory_space=pl.ANY)
    inside = pl.BlockSpec(memory_space=pltpu.VMEM)
    dma = pltpu.SemaphoreType.DMA
    out = pl.pallas_call(
        kernel,
        out_shape=jax.ShapeDtypeStruct((3, 2, 128), F32),
        in_specs=[anywhere] * 5,
        out_specs=inside,
        scratch_shapes=[
            pltpu.VMEM((320, 128), BF16),
            pltpu.VMEM((2, 320, 128), BF16),
            pltpu.VMEM((128,), jnp.int32),
            pltpu.VMEM((320,), F32),
            pltpu.VMEM((16, 8, 128), F32),
            pltpu.VMEM((GROUPS, 5, GTOK, 128), BF16),
            pltpu.VMEM((64 * GROUPS, 2, 5, GTOK, 128), BF16),
            pltpu.VMEM((2, 4, nwords, width // 4), BF16),
            pltpu.VMEM((256, width // 4), BF16),
            pltpu.VMEM((256, width // 4), BF16),
            pltpu.VMEM((256, width // 4), BF16),
            pltpu.VMEM((GROUPS, 2, 1200, 256), F32),
            pltpu.VMEM((2, 1200, 256), F32),
            pltpu.VMEM((GROUPS, 256, 128), F32),
            pltpu.VMEM((8, 256), F32),
            pltpu.VMEM((8, 256), F32),
            pltpu.VMEM((3, 8, 256), F32),
            pltpu.VMEM((GROUPS, 8, 128), F32),
            pltpu.VMEM((8, 4, 128), F32),
            pltpu.VMEM((8, 4, 128), F32),
            pltpu.VMEM((8, 128), F32),
            pltpu.VMEM((16, 8, 128), F32),
            dma((4,)),
            dma((4,)),
            dma((4,)),
            dma((4,)),
            dma((15,)),
            dma((15,)),
            dma,
            dma,
            dma((GROUPS,)),
            dma((63 * GROUPS,)),
            dma((8,)),
            dma((8,)),
            dma((16,)),
            dma((16,)),
        ],
        compiler_params=pltpu.CompilerParams(
            collective_id=0, has_side_effects=True, vmem_limit_bytes=60 * 1024 * 1024
        ),
    )(stream_in.T, deltas.transpose(0, 2, 1), norm_gain, unembed, targets)
    return out[0], out[1], out[2]


def solution(mesh):
    torus = Mesh(
        mesh.devices.reshape(mesh.shape["section"], 4, 4), ("section", "vocab_0", "vocab_1")
    )
    placed = (P(None, VOCAB), P("section", None, VOCAB), P(VOCAB), P(SECTION_VOCAB, None), P())
    return jax.shard_map(
        shards,
        mesh=torus,
        in_specs=placed,
        out_specs=(P("section", None), P("section", None), P("section", None)),
        check_vma=False,
    )
```

```python
import functools

import jax
import jax.numpy as jnp
from jax import lax
from jax.experimental import pallas as pl
from jax.experimental.pallas import tpu as pltpu
from jax.sharding import Mesh
from jax.sharding import PartitionSpec as P

MESH = pl.DeviceIdType.MESH
F32 = jnp.float32
BF16 = jnp.bfloat16
EPSILON = 1e-06

VOCAB = ("vocab_0", "vocab_1")
SECTION_VOCAB = ("section", "vocab_0", "vocab_1")

LINKS = ((0, 1), (0, -1), (1, 1), (1, -1), (2, 1), (2, -1))
TREE = (
    (-1, 0, 0, 1), (0, -1, 0, 3), (0, 0, -1, 5), (0, 0, 1, 4), (0, 1, 0, 2), (1, 0, 0, 0),
    (-1, -1, 0, 3), (-1, 0, -1, 1), (-1, 0, 1, 1), (-1, 1, 0, 1), (0, -1, -1, 5), (0, -1, 1, 4),
    (0, 0, 2, 4), (0, 1, -1, 5), (0, 1, 1, 2), (0, 2, 0, 2), (1, -1, 0, 0), (1, 0, -1, 0),
    (1, 0, 1, 0), (1, 1, 0, 0), (2, 0, 0, 0), (-1, -1, -1, 3), (-1, -1, 1, 1), (-1, 0, 2, 5),
    (-1, 1, -1, 5), (-1, 1, 1, 2), (-1, 2, 0, 1), (0, -1, 2, 3), (0, 1, 2, 4), (0, 2, -1, 3),
    (0, 2, 1, 2), (1, -1, -1, 0), (1, -1, 1, 4), (1, 0, 2, 4), (1, 1, -1, 2), (1, 1, 1, 2),
    (1, 2, 0, 3), (2, -1, 0, 0), (2, 0, -1, 0), (2, 0, 1, 1), (2, 1, 0, 2), (-1, -1, 2, 4),
    (-1, 1, 2, 5), (-1, 2, -1, 5), (-1, 2, 1, 3), (0, 2, 2, 5), (1, -1, 2, 5), (1, 1, 2, 4),
    (1, 2, -1, 3), (1, 2, 1, 3), (2, -1, -1, 0), (2, -1, 1, 1), (2, 0, 2, 5), (2, 1, -1, 2),
    (2, 1, 1, 2), (2, 2, 0, 3), (-1, 2, 2, 4), (1, 2, 2, 4), (2, -1, 2, 3), (2, 1, 2, 5),
    (2, 2, -1, 2), (2, 2, 1, 1), (2, 2, 2, 1),
)
PLAN = (
    (
        (1, 0, 0), (1, 1, 0), (1, 2, 0), (1, 3, 0), (1, 4, 0), (1, 5, 0), (1, 0, 1), (1, 1, 1), (1, 2, 1),
        (1, 3, 1), (1, 4, 1), (1, 5, 1), (1, 0, 2), (1, 1, 2), (1, 2, 2), (1, 3, 2), (1, 4, 2), (1, 5, 2),
        (1, 0, 3), (1, 1, 3), (1, 2, 3), (1, 3, 3), (1, 4, 3), (1, 5, 3), (0, 0, 0), (0, 1, 0), (0, 2, 0),
        (0, 3, 0), (0, 4, 0), (0, 5, 0), (1, 6, 0), (1, 8, 0), (1, 10, 0), (1, 11, 0), (1, 15, 0), (1, 16, 0),
        (1, 9, 0), (1, 17, 0), (0, 0, 1), (0, 1, 1), (0, 2, 1), (0, 3, 1), (0, 4, 1), (0, 5, 1), (1, 6, 1),
        (1, 10, 1), (1, 11, 1), (1, 15, 1), (1, 7, 0), (1, 18, 0), (0, 0, 2), (0, 1, 2), (0, 2, 2), (0, 3, 2),
        (0, 4, 2), (0, 5, 2), (1, 6, 2), (1, 10, 2), (1, 11, 2), (1, 15, 2), (1, 8, 1), (1, 16, 1), (0, 0, 3),
        (0, 1, 3), (0, 2, 3), (0, 3, 3), (0, 4, 3), (0, 5, 3), (1, 6, 3), (1, 10, 3), (1, 11, 3), (1, 15, 3),
        (1, 9, 1), (1, 12, 0), (1, 13, 0), (1, 14, 0), (1, 17, 1), (1, 13, 1), (1, 14, 1), (0, 6, 0), (0, 8, 0),
        (0, 10, 0), (0, 11, 0), (0, 15, 0), (0, 16, 0), (1, 22, 0), (1, 29, 0), (1, 31, 0), (1, 32, 0), (1, 12, 1),
        (1, 13, 2), (1, 14, 2), (0, 6, 1), (0, 9, 0), (0, 10, 1), (0, 11, 1), (0, 15, 1), (0, 17, 0), (1, 22, 1),
        (1, 29, 1), (1, 38, 0), (1, 24, 0), (1, 26, 0), (1, 12, 2), (1, 14, 3), (1, 18, 1), (0, 6, 2), (0, 7, 0),
        (0, 10, 2), (0, 11, 2), (0, 15, 2), (0, 18, 0), (1, 29, 2), (1, 12, 3), (1, 13, 3), (1, 16, 2), (1, 35, 0),
        (1, 39, 0), (0, 6, 3), (0, 8, 1), (0, 10, 3), (0, 11, 3), (0, 15, 3), (0, 16, 1), (1, 29, 3), (1, 22, 2),
        (1, 17, 2), (0, 9, 1), (0, 12, 0), (0, 13, 0), (0, 14, 0), (0, 17, 1), (1, 27, 0), (1, 28, 0), (1, 30, 0),
        (0, 29, 0), (1, 45, 0), (1, 7, 1), (1, 32, 1), (1, 19, 0), (0, 22, 0), (0, 13, 1), (0, 14, 1), (0, 31, 0),
        (0, 32, 0), (1, 44, 0), (1, 30, 1), (1, 49, 0), (0, 29, 1), (1, 45, 1), (1, 26, 1), (1, 28, 1), (1, 20, 0),
        (0, 22, 1), (0, 12, 1), (0, 13, 2), (0, 14, 2), (0, 38, 0), (1, 30, 2), (1, 27, 1), (0, 29, 2), (1, 45, 2),
        (1, 28, 2), (1, 37, 0), (1, 51, 0), (0, 24, 0), (0, 26, 0), (0, 12, 2), (0, 14, 3), (0, 18, 1), (1, 30, 3),
        (1, 27, 2), (0, 29, 3), (1, 45, 3), (1, 8, 2), (1, 28, 3), (1, 46, 0), (1, 38, 1), (1, 53, 0), (0, 12, 3),
        (0, 13, 3), (0, 16, 2), (0, 35, 0), (0, 39, 0), (1, 27, 3), (0, 27, 0), (1, 31, 1), (1, 34, 0), (1, 52, 0),
        (0, 22, 2), (0, 28, 0), (0, 30, 0), (0, 45, 0), (0, 17, 2),
    ),
    (
        (1, 44, 1), (0, 44, 0), (1, 56, 0), (1, 61, 0),
    ),
    (
        (1, 23, 0), (1, 9, 2), (1, 18, 2), (1, 35, 1), (1, 47, 0), (0, 7, 1), (0, 30, 1), (0, 45, 1), (0, 32, 1),
        (0, 19, 0), (1, 48, 0), (0, 49, 0),
    ),
    (
        (1, 25, 0), (1, 43, 0), (1, 16, 3), (1, 57, 0), (1, 39, 1), (0, 26, 1), (0, 28, 1), (0, 30, 2), (0, 45, 2),
        (0, 20, 0), (1, 36, 0), (0, 27, 1),
    ),
    (
        (1, 22, 3), (1, 42, 0), (1, 17, 3), (1, 33, 0), (1, 54, 0), (0, 28, 2), (0, 30, 3), (0, 45, 3), (0, 37, 0),
        (0, 51, 0), (1, 49, 1), (0, 27, 2),
    ),
    (
        (1, 41, 0), (1, 7, 2), (1, 24, 1), (1, 50, 0), (0, 8, 2), (0, 28, 3), (0, 46, 0), (0, 38, 1), (0, 53, 0),
        (1, 60, 0), (1, 21, 0), (0, 27, 3),
    ),
    (
        (1, 32, 2), (1, 19, 1), (1, 40, 0), (1, 59, 0), (0, 56, 0), (0, 31, 1), (0, 34, 0), (0, 52, 0), (0, 61, 0),
        (1, 62, 0), (1, 58, 0), (0, 44, 1),
    ),
    (
        (1, 26, 2), (1, 56, 1), (1, 46, 1), (1, 20, 1), (1, 53, 1), (0, 23, 0), (0, 9, 2), (0, 18, 2), (0, 35, 1),
        (0, 47, 0), (1, 55, 0), (0, 48, 0),
    ),
    (
        (1, 34, 1), (1, 47, 1), (1, 37, 1), (1, 51, 1), (1, 52, 1), (0, 25, 0), (0, 43, 0), (0, 16, 3), (0, 57, 0),
        (0, 39, 1), (1, 44, 2), (0, 36, 0), (1, 23, 1), (1, 35, 2), (1, 38, 2), (1, 61, 1), (0, 22, 3), (0, 42, 0),
        (0, 17, 3), (0, 33, 0), (0, 54, 0),
    ),
    (
        (1, 48, 1), (0, 49, 1), (1, 57, 1), (1, 8, 3), (1, 25, 1), (1, 43, 1), (1, 31, 2), (1, 33, 1), (0, 41, 0),
        (0, 7, 2), (0, 24, 1), (0, 50, 0), (0, 60, 0),
    ),
    (
        (1, 36, 1), (0, 21, 0), (1, 41, 1), (1, 9, 3), (1, 42, 1), (1, 18, 3), (1, 54, 1), (0, 32, 2), (0, 19, 1),
        (0, 40, 0), (0, 59, 0), (0, 62, 0), (1, 49, 2),
    ),
    (
        (0, 58, 0), (1, 24, 2), (1, 32, 3), (1, 50, 1), (0, 26, 2), (0, 56, 1), (0, 46, 1), (0, 20, 1), (0, 53, 1),
        (1, 60, 1), (1, 62, 1), (1, 21, 1), (0, 55, 0),
    ),
    (
        (1, 19, 2), (1, 39, 2), (1, 40, 1), (1, 59, 1), (0, 34, 1), (0, 47, 1), (0, 37, 1), (0, 51, 1), (0, 52, 1),
        (1, 58, 1), (0, 44, 2), (1, 56, 2),
    ),
    (
        (1, 7, 3), (1, 20, 2), (0, 23, 1), (0, 35, 2), (0, 57, 1), (0, 38, 2), (0, 61, 1), (1, 47, 2), (1, 52, 2),
        (1, 53, 2), (1, 55, 1), (0, 48, 1),
    ),
    (
        (1, 26, 3), (1, 33, 2), (1, 34, 2), (1, 37, 2), (0, 8, 3), (0, 25, 1), (0, 43, 1), (0, 31, 2), (0, 33, 1),
        (1, 46, 2), (1, 44, 3), (0, 36, 1),
    ),
    (
        (1, 23, 2), (1, 51, 2), (1, 38, 3), (0, 41, 1), (0, 9, 3), (0, 42, 1), (0, 18, 3), (0, 54, 1), (1, 35, 3),
        (1, 48, 2), (0, 49, 2), (1, 57, 2),
    ),
    (
        (1, 41, 2), (1, 25, 2), (1, 43, 2), (1, 31, 3), (1, 61, 2), (0, 24, 2), (0, 32, 3), (0, 50, 1), (0, 60, 1),
        (0, 62, 1), (1, 36, 2), (0, 21, 1),
    ),
    (
        (1, 42, 2), (1, 33, 3), (1, 50, 2), (0, 56, 2), (0, 19, 2), (0, 39, 2), (0, 40, 1), (0, 59, 1), (1, 54, 2),
        (1, 62, 2), (1, 49, 3), (0, 58, 1),
    ),
    (
        (1, 41, 3), (1, 24, 3), (1, 19, 3), (1, 39, 3), (0, 7, 3), (0, 47, 2), (0, 20, 2), (0, 52, 2), (0, 53, 2),
        (1, 60, 2), (1, 21, 2), (0, 55, 1), (1, 51, 3), (1, 20, 3), (1, 40, 2), (1, 59, 2),
    ),
    (
        (0, 26, 3), (0, 46, 2), (0, 33, 2), (0, 34, 2), (0, 37, 2), (1, 58, 2), (0, 44, 3), (1, 56, 3), (1, 37, 3),
        (1, 61, 3), (0, 23, 2), (0, 35, 3), (0, 57, 2), (0, 51, 2), (0, 38, 3),
    ),
    (
        (1, 47, 3), (1, 52, 3), (1, 53, 3), (1, 55, 2), (0, 48, 2), (1, 34, 3), (0, 41, 2), (0, 25, 2), (0, 43, 2),
        (0, 31, 3), (0, 61, 2), (1, 46, 3), (1, 50, 3), (1, 48, 3), (0, 36, 2),
    ),
    (
        (1, 23, 3), (1, 25, 3), (0, 42, 2), (0, 33, 3), (0, 50, 2), (0, 54, 2), (0, 62, 2), (1, 36, 3), (0, 49, 3),
        (1, 57, 3),
    ),
    (
        (1, 43, 3), (0, 41, 3), (0, 24, 3), (0, 19, 3), (0, 39, 3), (0, 60, 2), (1, 54, 3), (1, 21, 3), (0, 21, 2),
    ),
    (
        (1, 42, 3), (0, 56, 3), (0, 51, 3), (0, 20, 3), (0, 40, 2), (0, 59, 2), (1, 40, 3), (1, 62, 3), (0, 58, 2),
    ),
    (
        (0, 47, 3), (0, 37, 3), (0, 52, 3), (0, 53, 3), (0, 61, 3), (1, 58, 3), (1, 59, 3), (1, 60, 3), (1, 55, 3),
        (0, 55, 2),
    ),
    (
        (0, 46, 3), (0, 34, 3), (0, 50, 3), (0, 48, 3), (0, 57, 3),
    ),
    (
        (0, 23, 3), (0, 25, 3), (0, 36, 3),
    ),
    (
        (0, 43, 3), (0, 54, 3), (0, 21, 3), (0, 62, 3),
    ),
    (
        (0, 42, 3), (0, 40, 3), (0, 58, 3),
    ),
    (
        (0, 59, 3), (0, 60, 3), (0, 55, 3),
    ),
    (),
    (),
    (),
    (),
    (),
)
PLANES = (0, 1, -1, 2)

GROUPS = 4
GTOK = 16
FILL = -1e30


def dispatch(index, branches, low=0, high=None):
    high = len(branches) if high is None else high
    if not any(branches[low:high]):
        return
    if high - low == 1:
        branches[low]()
        return
    mid = (low + high) // 2

    @pl.when(index < mid)
    def _():
        dispatch(index, branches, low, mid)

    @pl.when(index >= mid)
    def _():
        dispatch(index, branches, mid, high)


def kernel(
    stream_hbm, deltas_hbm, gain_hbm, unembed_hbm, targets_hbm, out_ref,
    stream_v, deltas_v, targets_v, gain_v, gains, outbox, gat, words, rows_a, rows_b, rows_c, acc, final,
    squares, scales, tops, sums, stats, slices, from_section, partial, from_plane,
    load_sem, own_sem, words_send, words_recv, gain_send, gain_recv,
    part_send, part_recv, send_sem, recv_sem,
    section_send, section_recv, plane_send, plane_recv,
):
    section = lax.axis_index("section")
    x = lax.axis_index("vocab_0")
    z = lax.axis_index("vocab_1")
    y = section // 2
    core = section % 2
    sign = 1 - 2 * core
    nwords = unembed_hbm.shape[0]
    plane_width = unembed_hbm.shape[1] // 4
    home = (x, y, z)

    def device(xx, yy, zz, cc):
        return (yy * 2 + cc, xx, zz)

    def moved(axis, step):
        at = list(home)
        at[axis] = lax.rem(at[axis] + step + 4, 4)
        return tuple(at)

    neighbours = [device(*moved(axis, way * sign), core) for axis, way in LINKS]
    partner = device(x, y, z, 1 - core)
    source = [{d: lax.rem(home[axis] - sign * d + 4, 4) for d in (-1, 0, 1, 2)} for axis in range(3)]

    loads = [
        pltpu.make_async_copy(stream_hbm, stream_v, load_sem.at[0]),
        pltpu.make_async_copy(deltas_hbm, deltas_v, load_sem.at[1]),
        pltpu.make_async_copy(targets_hbm, targets_v, load_sem.at[2]),
        pltpu.make_async_copy(gain_hbm, gain_v, load_sem.at[3]),
    ]
    for copy in loads:
        copy.start()

    def plane_peer(step):
        return device(lax.rem(x + step // 4, 4), y, lax.rem(z + step % 4, 4), core)

    def section_peer(step, other):
        return device(x, lax.rem(y + step, 4), z, 1 - core if other else core)

    section_peers = [(step, other) for step in range(4) for other in (0, 1) if step or other]
    barrier = pltpu.get_barrier_semaphore()
    around = [device(*moved(axis, way), cc) for axis, way in LINKS for cc in range(2)]
    for peer in around + [partner]:
        pl.semaphore_signal(barrier, inc=1, device_id=peer, device_id_type=MESH)

    def columns(plane):
        return pl.ds(pl.multiple_of(plane * plane_width, 128), plane_width)

    own_words = []
    for p, dx in enumerate(PLANES):
        plane = source[0][dx]
        own_words.append(
            pltpu.make_async_copy(
                unembed_hbm.at[:, columns(plane)], words.at[0, plane, pl.ds(0, nwords)], own_sem.at[p]
            )
        )
        own_words[-1].start()

    for copy in loads:
        copy.wait()

    lane = lax.broadcasted_iota(jnp.int32, (GTOK, 128), 1)
    low = lane < 64
    odd = lax.rem(z, 2) == 1
    my_slot = ((x * 4 + y) * 4 + z) * GROUPS

    first = jnp.where(section == 0, 1.0, 0.0).astype(F32)
    former = deltas_v[0].astype(F32) + stream_v[...].astype(F32) * first
    kept = former.astype(BF16).astype(F32)
    latter = deltas_v[1].astype(F32) + (former - kept)
    packed = []
    heads = []
    for value in (kept, latter):
        packed.append(jnp.where(odd, value[64:192], value[0:128]))
        packed.append(jnp.where(odd, value[192:320], value[128:256]))
        heads.append(jnp.where(odd, value[0:64], value[256:320]))
    lead = jnp.where(odd, heads[1], heads[0])
    trail = jnp.where(odd, heads[0], heads[1])
    packed.append(jnp.concatenate([lead, trail], axis=0))
    for k, value in enumerate(packed):
        tile = jnp.transpose(value).astype(BF16)
        for half in range(2):

            @pl.when(core == half)
            def _():
                for g in range(GROUPS):
                    t0 = half * 64 + g * GTOK
                    gat[my_slot + g, core, k] = tile[t0 : t0 + GTOK]

            @pl.when(core != half)
            def _():
                for g in range(GROUPS):
                    t0 = half * 64 + g * GTOK
                    outbox[g, k] = tile[t0 : t0 + GTOK]

    low_row = lax.broadcasted_iota(jnp.int32, (1, 128), 1) < 64
    none = jnp.zeros((1, 64), F32)
    g0 = gain_v[0:128].reshape(1, 128)
    g1 = gain_v[128:256].reshape(1, 128)
    g2 = jnp.concatenate([gain_v[256:320].reshape(1, 64), none], axis=1)
    t0, t1, t2 = (pltpu.roll(v, 64, 1) for v in (g0, g1, g2))
    blank = jnp.zeros((1, 128), F32)
    gain_rows = (
        (g0, blank),
        (g1, blank),
        (g2, jnp.where(low_row, 0.0, t0)),
        (blank, jnp.where(low_row, t0, t1)),
        (blank, jnp.where(low_row, t1, t2)),
    )
    gains[x * 4 + z] = jnp.concatenate(
        [jnp.where(odd, other, even) for even, other in gain_rows] + [blank] * 3, axis=0
    )

    final[:, 1184:1200, :] = jnp.full((2, 16, 256), FILL, F32)

    pl.semaphore_wait(barrier, 13)

    part = pltpu.make_async_remote_copy(
        src_ref=outbox,
        dst_ref=gat.at[pl.ds(my_slot, GROUPS), core],
        send_sem=part_send,
        recv_sem=part_recv,
        device_id=partner,
        device_id_type=MESH,
    )
    part.start()

    def gain_copy(n, link):
        at = (source[0][n[0]] * 4 + source[2][n[2]])
        place = (TREE_INDEX[child(n, link)] if link is not None else TREE_INDEX[n])
        return pltpu.make_async_remote_copy(
            src_ref=gains.at[at],
            dst_ref=gains.at[at],
            send_sem=gain_send.at[GAIN_INDEX[place]],
            recv_sem=gain_recv.at[GAIN_INDEX[place]],
            device_id=neighbours[link or 0],
            device_id_type=MESH,
        )

    def block_copy(n, row, link, g):
        slot = source[0][n[0]] * 64 + source[1][n[1]] * 16 + source[2][n[2]] * 4 + g
        return pltpu.make_async_remote_copy(
            src_ref=gat.at[slot],
            dst_ref=gat.at[slot],
            send_sem=send_sem.at[g],
            recv_sem=recv_sem.at[row * GROUPS + g],
            device_id=neighbours[link],
            device_id_type=MESH,
        )

    def first_copy(row, link, g, away):
        axis, way = LINKS[link]
        return pltpu.make_async_remote_copy(
            src_ref=outbox.at[g] if away else gat.at[my_slot + g, core],
            dst_ref=gat.at[my_slot + g, core],
            send_sem=send_sem.at[g],
            recv_sem=recv_sem.at[row * GROUPS + g],
            device_id=device(*moved(axis, -way * sign), 1 - core) if away else neighbours[link],
            device_id_type=MESH,
        )

    def send_gain(n):
        for row, (dx, dy, dz, link) in enumerate(TREE):
            if dy == 0 and parent((dx, dy, dz), link) == n:
                gain_copy(n, link).start()

    def run(actions):
        for kind, row, g in actions:
            dx, dy, dz, link = TREE[row]
            n = (dx, dy, dz)
            if kind == 0:
                block_copy(n, row, link, g).wait_recv()
                if g == 0 and dy == 0:
                    gain_copy(n, None).wait_recv()
                    send_gain(n)
            elif parent(n, link) == (0, 0, 0):
                for away in (False, True):
                    first_copy(row, link, g, away).start()
            else:
                block_copy(parent(n, link), row, link, g).start()

    send_gain((0, 0, 0))

    their_words = []
    for p, dx in enumerate(PLANES):
        plane = lax.rem(x + sign * dx + 4, 4)
        their_words.append(
            pltpu.make_async_remote_copy(
                src_ref=unembed_hbm.at[:, columns(plane)],
                dst_ref=words.at[1, plane, pl.ds(0, nwords)],
                send_sem=words_send.at[p],
                recv_sem=words_recv.at[p],
                device_id=partner,
                device_id_type=MESH,
            )
        )

    for copy in their_words[:2]:
        copy.start()

    segment = lax.broadcasted_iota(jnp.int32, (1, 128), 1) // GTOK

    def spread(value):
        for step in (16, 32, 64):
            value = value + pltpu.roll(value, step, 1)
        return value

    def prepare(g, p, zp, rows):
        plane = source[0][PLANES[p]]
        running = [jnp.zeros((GTOK, 128), F32) for _ in range(5)]
        both = gains[plane * 4 + 2 * zp] + gains[plane * 4 + 2 * zp + 1]
        factor = [jnp.broadcast_to(both[k : k + 1, :], (GTOK, 128)) for k in range(5)]
        for yy in range(4):
            even = plane * 64 + yy * 16 + 2 * zp * 4 + g
            other = even + 4
            for cc in range(2):
                pe = gat[even, cc, 4].astype(F32)
                po = gat[other, cc, 4].astype(F32)
                for l in range(2):
                    layer = 4 * yy + 2 * cc + l
                    if l == 0:
                        middle = jnp.where(low, pe, po)
                    else:
                        middle = pltpu.roll(jnp.where(low, po, pe), 64, 1)
                    values = [
                        gat[even, cc, 2 * l].astype(F32),
                        gat[even, cc, 2 * l + 1].astype(F32),
                        middle,
                        gat[other, cc, 2 * l].astype(F32),
                        gat[other, cc, 2 * l + 1].astype(F32),
                    ]
                    span = slice(layer * GTOK, (layer + 1) * GTOK)
                    total = jnp.zeros((GTOK, 128), F32) if p == 0 and zp == 0 else squares[g, span, :]
                    for k in range(5):
                        at = 5 * zp + k
                        running[k] = running[k] + values[k]
                        total = total + running[k] * running[k]
                        rows[span, at * 128 : (at + 1) * 128] = (running[k] * factor[k]).astype(BF16)
                    squares[g, span, :] = total

    def multiply(g, p, stretch, rows):
        start, stop = ((0, 592), (592, nwords))[stretch]
        plane = source[0][PLANES[p]]
        most = []
        for half in range(2):
            product = lax.dot_general(
                words[half, plane, start:stop, :], rows[...], (((1,), (1,)), ((), ())), preferred_element_type=F32
            )
            if p == 0:
                acc[g, half, start:stop, :] = product
            elif p < 3:
                acc[g, half, start:stop, :] = acc[g, half, start:stop, :] + product
            else:
                total = acc[g, half, start:stop, :] + product
                final[half, start:stop, :] = total
                most.append(jnp.max(total[0:592].reshape(74, 8, 256), axis=0))
                if stop - start > 592:
                    most.append(jnp.broadcast_to(jnp.max(total[592:], axis=0, keepdims=True), (8, 256)))
        if p == 3:
            if stretch == 1:
                most.append(tops[...])
            tops[...] = functools.reduce(jnp.maximum, most)

    def scaled(g):
        total = jnp.sum(jnp.transpose(squares[g]), axis=0, keepdims=True)
        scales[0:1, :] = lax.rsqrt(total / (4 * plane_width) + EPSILON)

    def peaked():
        scales[1:2, :] = jnp.max(tops[...], axis=0, keepdims=True) * scales[0:1, :]

    def folded(g, piece):
        half = piece // 2
        scale = jnp.broadcast_to(scales[0:1, :], (8, 256))
        peaks = jnp.broadcast_to(scales[1:2, :], (8, 256))
        sublane = lax.broadcasted_iota(jnp.int32, (8, 256), 0)
        holder = core if half == 0 else 1 - core
        first_word = (((y * 2 + holder) * 4 + x) * 4 + z) * nwords
        local = targets_v[...].reshape(1, 128) - first_word
        local = jnp.where(local < nwords, local, -8)
        local = spread(jnp.where(segment == core * GROUPS + g, local, 0))
        wanted = jnp.broadcast_to(jnp.concatenate([local, local], axis=1), (8, 256)) - sublane
        if piece == 0:
            mass = moment = picked = jnp.zeros((8, 256), F32)
        else:
            mass, moment, picked = (sums[k] for k in range(3))
        for k in range(75 * (piece % 2), 75 * (piece % 2) + 75):
            z_all = final[half, 8 * k : 8 * k + 8, :] * scale
            z_rel = z_all - peaks
            e = jnp.exp(z_rel)
            mass = mass + e
            moment = moment + e * z_rel
            picked = jnp.where(wanted == 8 * k, z_all, picked)
        if piece < 3:
            for k, value in enumerate((mass, moment, picked)):
                sums[k] = value
            return
        found = [scales[1:2, :]] + [jnp.sum(v, axis=0, keepdims=True) for v in (mass, moment, picked)]
        for k, value in enumerate(found):
            stats[g, 2 * k : 2 * k + 1, :] = value[:, 0:128]
            stats[g, 2 * k + 1 : 2 * k + 2, :] = value[:, 128:256]

    def words_ready(p):
        plane = source[0][PLANES[p]]
        own_words[p].wait()
        pltpu.make_async_remote_copy(
            src_ref=unembed_hbm.at[:, columns(plane)],
            dst_ref=words.at[1, plane, pl.ds(0, nwords)],
            send_sem=words_send.at[p],
            recv_sem=words_recv.at[p],
            device_id=partner,
            device_id_type=MESH,
        ).wait_recv()

    run(PLAN[0])
    for copy in their_words[2:]:
        copy.start()
    part.wait_recv()
    for zp in range(2):
        prepare(0, 0, zp, rows_c)
    run(PLAN[1])
    words_ready(0)
    multiply(0, 0, 0, rows_c)
    run(PLAN[2])
    multiply(0, 0, 1, rows_c)
    run(PLAN[3])
    for zp in range(2):
        prepare(1, 0, zp, rows_a)
    for g, now, later in ((1, rows_a, rows_b), (2, rows_b, rows_c), (3, rows_c, rows_a)):
        for k in range(2):
            run(PLAN[2 + 2 * g + k])
            multiply(g, 0, k, now)
            prepare(*((g + 1, 0) if g < 3 else (0, 1)), k, later)

    def body(g, carry):
        rotation = (rows_a, rows_b, rows_c)
        for p in (1, 2, 3):
            now, later = rotation[p - 1], rotation[p % 3]
            following = (g, p + 1) if p < 3 else (jnp.minimum(g + 1, GROUPS - 1), 1)
            former_group = lax.rem(g + GROUPS - 1, GROUPS)
            if p == 3:
                scaled(g)
            for k in range(2):
                rows_of_plan = [PLAN[10 + 6 * j + 2 * (p - 1) + k] for j in range(GROUPS)]
                dispatch(g, [functools.partial(run, row) if row else None for row in rows_of_plan])
                if k == 0:
                    pl.when(g == 0)(functools.partial(words_ready, p))
                multiply(g, p, k, now)
                prepare(*following, k, later)
                if p < 3:
                    folded(former_group, 2 * (p - 1) + k)
            if p == 3:
                peaked()
        return carry

    lax.fori_loop(0, GROUPS, body, 0)
    run(PLAN[34])
    for piece in range(4):
        folded(GROUPS - 1, piece)

    def joined(parts):
        most = functools.reduce(jnp.maximum, [part[0] for part in parts])
        shifts = [part[0] - most for part in parts]
        factors = [jnp.exp(shift) for shift in shifts]
        mass = sum(f * part[1] for f, part in zip(factors, parts))
        moment = sum(f * (part[2] + shift * part[1]) for f, shift, part in zip(factors, shifts, parts))
        return most, mass, moment, sum(part[3] for part in parts)

    wide_segment = lax.broadcasted_iota(jnp.int32, (8, 128), 1) // 32
    for q in range(4):
        value = jnp.zeros((8, 128), F32)
        for g in range(GROUPS):
            shift = 32 * ((g - q) % 4)
            moved_row = pltpu.roll(stats[g], shift, 1) if shift else stats[g]
            value = jnp.where(wide_segment == g, moved_row, value)
        for half in range(2):
            for k in range(4):
                slices[half * 4 + q, k : k + 1, :] = value[2 * k + half : 2 * k + half + 1, :]

    def section_copy(step, other):
        yy = lax.rem(y + step, 4)
        cc = 1 - core if other else core
        at = step * 2 + other
        return pltpu.make_async_remote_copy(
            src_ref=slices.at[yy * 2 + cc],
            dst_ref=from_section.at[at],
            send_sem=section_send.at[at],
            recv_sem=section_recv.at[at],
            device_id=section_peer(step, other),
            device_id_type=MESH,
        )

    for p in section_peers:
        section_copy(*p).start()
    from_section[0] = slices[section]
    for p in section_peers:
        section_copy(*p).wait_recv()
    for other in range(2):
        arrived = [from_section[2 * step + other] for step in range(4)]
        found = joined([[part[k : k + 1] for k in range(4)] for part in arrived])
        for k, value in enumerate(found):
            row = 4 * (core if other == 0 else 1 - core) + k
            partial[pl.ds(row, 1), :] = value

    def plane_copy(step):
        return pltpu.make_async_remote_copy(
            src_ref=partial,
            dst_ref=from_plane.at[step],
            send_sem=plane_send.at[step],
            recv_sem=plane_recv.at[step],
            device_id=plane_peer(step),
            device_id_type=MESH,
        )

    for step in range(1, 16):
        plane_copy(step).start()
    from_plane[0] = partial[...]
    for step in range(1, 16):
        plane_copy(step).wait_recv()
    everything = [from_plane[step] for step in range(16)]
    narrow = lax.broadcasted_iota(jnp.int32, (1, 128), 1)
    result = [[jnp.zeros((1, 128), F32) for _ in range(2)] for _ in range(3)]
    for half in range(2):
        most, mass, moment, picked = joined([[part[4 * half + k : 4 * half + k + 1] for k in range(4)] for part in everything])
        log_mass = jnp.log(mass)
        lse = most + log_mass
        for n, value in enumerate((lse, log_mass - moment / mass, picked - lse)):
            for l in range(2):
                for g in range(GROUPS):
                    shift = (64 * half + 16 * g - 32 * g - 16 * l) % 128
                    moved_row = pltpu.roll(value, shift, 1) if shift else value
                    result[n][l] = jnp.where(narrow // GTOK == 4 * half + g, moved_row, result[n][l])
    for n in range(3):
        for l in range(2):
            out_ref[n, l : l + 1, :] = result[n][l]

    for p in section_peers:
        section_copy(*p).wait_send()
    for step in range(1, 16):
        plane_copy(step).wait_send()
    part.wait_send()
    for copy in their_words:
        copy.wait_send()
    for row, (dx, dy, dz, link) in enumerate(TREE):
        if dy == 0:
            gain_copy(parent((dx, dy, dz), link), link).wait_send()
    for g in range(GROUPS):
        pltpu.make_async_remote_copy(
            src_ref=gat.at[pl.ds(0, len(TREE))],
            dst_ref=gat.at[pl.ds(0, len(TREE))],
            send_sem=send_sem.at[g],
            recv_sem=recv_sem.at[0],
            device_id=neighbours[0],
            device_id_type=MESH,
        ).wait_send()


def wrapped(c):
    return (c + 1) % 4 - 1


def parent(n, link):
    axis, way = LINKS[link]
    n = list(n)
    n[axis] = wrapped(n[axis] - way)
    return tuple(n)


def child(n, link):
    axis, way = LINKS[link]
    n = list(n)
    n[axis] = wrapped(n[axis] + way)
    return tuple(n)


TREE_INDEX = {row[:3]: k for k, row in enumerate(TREE)}
GAIN_INDEX = {k: i for i, k in enumerate(k for k, row in enumerate(TREE) if row[1] == 0)}


def shards(stream_in, deltas, norm_gain, unembed, targets):
    nwords, width = unembed.shape
    anywhere = pl.BlockSpec(memory_space=pl.ANY)
    inside = pl.BlockSpec(memory_space=pltpu.VMEM)
    dma = pltpu.SemaphoreType.DMA
    out = pl.pallas_call(
        kernel,
        out_shape=jax.ShapeDtypeStruct((3, 2, 128), F32),
        in_specs=[anywhere] * 5,
        out_specs=inside,
        scratch_shapes=[
            pltpu.VMEM((320, 128), BF16),
            pltpu.VMEM((2, 320, 128), BF16),
            pltpu.VMEM((128,), jnp.int32),
            pltpu.VMEM((320,), F32),
            pltpu.VMEM((16, 8, 128), F32),
            pltpu.VMEM((GROUPS, 5, GTOK, 128), BF16),
            pltpu.VMEM((64 * GROUPS, 2, 5, GTOK, 128), BF16),
            pltpu.VMEM((2, 4, nwords, width // 4), BF16),
            pltpu.VMEM((256, width // 4), BF16),
            pltpu.VMEM((256, width // 4), BF16),
            pltpu.VMEM((256, width // 4), BF16),
            pltpu.VMEM((GROUPS, 2, 1200, 256), F32),
            pltpu.VMEM((2, 1200, 256), F32),
            pltpu.VMEM((GROUPS, 256, 128), F32),
            pltpu.VMEM((8, 256), F32),
            pltpu.VMEM((8, 256), F32),
            pltpu.VMEM((3, 8, 256), F32),
            pltpu.VMEM((GROUPS, 8, 128), F32),
            pltpu.VMEM((8, 4, 128), F32),
            pltpu.VMEM((8, 4, 128), F32),
            pltpu.VMEM((8, 128), F32),
            pltpu.VMEM((16, 8, 128), F32),
            dma((4,)),
            dma((4,)),
            dma((4,)),
            dma((4,)),
            dma((15,)),
            dma((15,)),
            dma,
            dma,
            dma((GROUPS,)),
            dma((63 * GROUPS,)),
            dma((8,)),
            dma((8,)),
            dma((16,)),
            dma((16,)),
        ],
        compiler_params=pltpu.CompilerParams(
            collective_id=0, has_side_effects=True, vmem_limit_bytes=60 * 1024 * 1024
        ),
    )(stream_in.T, deltas.transpose(0, 2, 1), norm_gain, unembed, targets)
    return out[0], out[1], out[2]


def solution(mesh):
    torus = Mesh(
        mesh.devices.reshape(mesh.shape["section"], 4, 4), ("section", "vocab_0", "vocab_1")
    )
    placed = (P(None, VOCAB), P("section", None, VOCAB), P(VOCAB), P(SECTION_VOCAB, None), P())
    return jax.shard_map(
        shards,
        mesh=torus,
        in_specs=placed,
        out_specs=(P("section", None), P("section", None), P("section", None)),
        check_vma=False,
    )
```
